32 devices in a mesh: tm: 8 (over y, x, core), diag: 4 (over z).
Axes of the slice: x: 2, y: 2, z: 4, core: 2. Of those that a mesh axis runs over, the one named last changes fastest.
Arguments:
- series: float32 [131072], P('tm'), may hold values from -6 to 6
- tail: float32 [256], replicated, may hold values from -6 to 6
- diag_offsets: int32 [4], P('diag'), may hold values from 0 to 12000, as said below
- exclusion: int32 [1], replicated, may hold values from 64 to 255
Outputs:
- profile: float32 [131072], P(('tm', 'diag'))
The draws below stay inside these ranges and needn't reach their ends.
Inputs may be any that keep to these rules, and one draw needn't show every extreme that they name: `diag_offsets`: in every draw some group starts at 12000 and another below 64; the others anywhere in the range, blocks may intersect.
All inputs are finite; a program needn't handle non-finite values.
Results may differ from the reference program's by a relative error of at most 0.0003.
Values sent between devices are 32-bit elements; how exact they have to be, the bound alone decides.
No kernel may reach another device: no remote copies, remote signals or barrier semaphores. Data moves between devices by JAX's collectives and lax.ppermute only.
A program may use at most 64 MiB of HBM per device.

```python
import jax
import jax.numpy as jnp
from jax import lax

M = 256
KB = 32
RB = 8192
REACH = 12288
SERIES = 131072
N_TM = 8
N_DIAG = 4


def draw_diag_offsets(key, part):
    highest = REACH - KB - M
    keys = jax.random.split(jax.random.fold_in(key, 17), 3)
    drawn = jax.random.randint(keys[0], (N_DIAG,), 0, highest + 1)
    chosen = jax.random.permutation(keys[1], N_DIAG)
    shallow = jax.random.randint(keys[2], (), 0, M // 4)
    group_ids = jnp.arange(N_DIAG)
    drawn = jnp.where(group_ids == chosen[0], highest, drawn)
    drawn = jnp.where(group_ids == chosen[1], shallow, drawn)
    return drawn.astype(jnp.int32)


def shard_levels(rng, extent, shards, smallest, top_value):
    def one(position, blocks):
        draws = jax.random.uniform(jax.random.fold_in(jax.random.fold_in(rng, 6), position), (blocks,), jnp.float32, smallest / len(shards), top_value / len(shards))
        return jnp.repeat(jnp.exp(draws), extent[position] // blocks).reshape((-1,) + (1,) * (len(extent) - position - 1))

    loudness = one(*shards[0])
    for cut in shards[1:]:
        loudness = loudness * one(*cut)
    return loudness


def gaussian(stream_key, dims, scale, most, cuts=(), held_as=jnp.bfloat16):
    values = jax.random.normal(stream_key, dims, jnp.float32) * scale
    if len(cuts) > 0:
        values = shard_levels(stream_key, dims, cuts, -0.22, 0.18) * values
    return jnp.clip(values, min=-most, max=most).astype(held_as)


def setup_inputs(seed: int = 0) -> dict:
    arg_keys = jax.random.split(jax.random.key(seed), 5)
    return {
        "series": gaussian(arg_keys[0], (SERIES,), 1.0, 6.0, ((0, 8),), jnp.float32),
        "tail": gaussian(arg_keys[1], (M,), 1.0, 6.0, (), jnp.float32),
        "diag_offsets": draw_diag_offsets(jax.random.fold_in(arg_keys[4], 71), 0),
        "exclusion": jax.random.randint(arg_keys[3], (1,), M // 4, M).astype(jnp.int32),
    }


FILL = 1e+30

def window_stats(extended):
    count = extended.shape[0] // M
    blocks = jnp.concatenate([extended, jnp.zeros((M,), jnp.float32)]).reshape(count + 1, M)
    row_ids = lax.broadcasted_iota(jnp.int32, (M, M), 0)
    col_ids = lax.broadcasted_iota(jnp.int32, (M, M), 1)
    upper = (row_ids >= col_ids).astype(jnp.float32)
    lower = (row_ids < col_ids).astype(jnp.float32)

    def window_sums(values):
        head = jnp.dot(values[:-1], upper, precision=lax.Precision.HIGHEST, preferred_element_type=jnp.float32)
        after = jnp.dot(values[1:], lower, precision=lax.Precision.HIGHEST, preferred_element_type=jnp.float32)
        return (head + after).reshape(-1)
    first = window_sums(blocks) / M
    second = window_sums(blocks * blocks) / M
    return (first, 1.0 / jnp.sqrt(second - first * first + 1e-05))

def hankel(vector, height, width):
    span = height + width
    tiled = jnp.tile(vector[:span], height + 1)[:height * (span + 1)]
    return tiled.reshape(height, span + 1)[:, :width]

def skew(matrix):
    height, width = matrix.shape
    padded = jnp.concatenate([matrix, jnp.full((height, height), FILL, matrix.dtype)], axis=1)
    flat = padded.reshape(-1)[:height * (width + height - 1)]
    return flat.reshape(height, width + height - 1)

def running_sums(values):
    height, width = values.shape
    inner = 128 if width % 128 == 0 else width
    grouped = values.reshape(height, width // inner, inner)
    within = jnp.cumsum(grouped, axis=2) - grouped
    totals = lax.optimization_barrier(jnp.sum(grouped, axis=2))
    before = jnp.cumsum(totals, axis=1) - totals
    return ((within + before[:, :, None]).reshape(height, width), lax.optimization_barrier(jnp.sum(totals, axis=1)))

def block_terms(extended, offset, row_start, rows):
    leading = lax.dynamic_slice_in_dim(extended, row_start, rows + M)
    partner = hankel(lax.dynamic_slice_in_dim(extended, row_start + offset, KB + rows + M), KB, rows + M)
    return leading[None, M:] * partner[:, M:] - leading[None, :rows] * partner[:, :rows]

def first_products(extended, offset):
    partner = hankel(lax.dynamic_slice_in_dim(extended, offset, KB + M), KB, M)
    return jnp.dot(partner, extended[:M], precision=lax.Precision.HIGHEST, preferred_element_type=jnp.float32)

def sweep(extended, means, spreads, offset, exclusion_width, limit, start, segment):
    rows = min(RB, segment)
    diag_ids = lax.broadcasted_iota(jnp.int32, (KB, rows), 0)
    row_ids = lax.broadcasted_iota(jnp.int32, (KB, rows), 1)

    def advance(index, carry):
        current, row_best, column_best = carry
        row_start = (index * rows).astype(jnp.int32)
        change = block_terms(extended, offset, row_start, rows)
        running, total = running_sums(change)
        products = current[:, None] + running
        mean_row = lax.dynamic_slice_in_dim(means, row_start, rows)
        spread_row = lax.dynamic_slice_in_dim(spreads, row_start, rows)
        mean_pair = hankel(lax.dynamic_slice_in_dim(means, row_start + offset, KB + rows), KB, rows)
        spread_pair = hankel(lax.dynamic_slice_in_dim(spreads, row_start + offset, KB + rows), KB, rows)
        corr = (products / M - mean_row[None, :] * mean_pair) * (spread_row[None, :] * spread_pair)
        distance = jnp.sqrt(1.0 - corr)
        partner_pos = row_start + offset + diag_ids + row_ids
        counted = (offset + diag_ids >= exclusion_width) & (partner_pos < limit)
        masked = jnp.where(counted, distance, FILL)
        row_best = lax.dynamic_update_slice_in_dim(row_best, lax.optimization_barrier(jnp.min(masked, axis=0)), row_start, 0)
        column_block = lax.optimization_barrier(jnp.min(skew(masked), axis=0))
        column_start = (row_start + offset).astype(jnp.int32)
        previous = lax.dynamic_slice_in_dim(column_best, column_start, rows + KB - 1)
        column_best = lax.dynamic_update_slice_in_dim(column_best, jnp.minimum(previous, column_block), column_start, 0)
        return (current + total, row_best, column_best)
    initial = (start, jnp.full((segment,), FILL, jnp.float32), jnp.full((extended.shape[0],), FILL, jnp.float32))
    result = lax.fori_loop(0, segment // rows, advance, initial)
    return (result[1], result[2])

def reference(series, tail, diag_offsets, exclusion):
    total_points = series.shape[0]
    segment = total_points // N_TM
    reach = segment // 2 + segment // 4
    padded_series = jnp.concatenate([series, tail, jnp.zeros((reach - M,), jnp.float32)])
    means, spreads = window_stats(padded_series)
    exclusion_width = exclusion[0].astype(jnp.int32)
    profile_best = jnp.full((total_points,), FILL, jnp.float32)
    for group in range(N_DIAG):
        offset = diag_offsets[group].astype(jnp.int32)

        def one_segment(place):
            begin = (place * segment).astype(jnp.int32)
            extended = lax.dynamic_slice_in_dim(padded_series, begin, segment + reach)
            local_means = lax.dynamic_slice_in_dim(means, begin, segment + reach)
            local_spreads = lax.dynamic_slice_in_dim(spreads, begin, segment + reach)
            limit = jnp.where(place == N_TM - 1, segment, segment + reach).astype(jnp.int32)
            start = first_products(extended, offset)
            row_best, column_best = sweep(extended, local_means, local_spreads, offset, exclusion_width, limit, start, segment)
            return (jnp.minimum(row_best, column_best[:segment]), column_best[segment:])
        owned, upper = lax.map(one_segment, jnp.arange(N_TM, dtype=jnp.int32))
        spilled = jnp.concatenate([jnp.full((1, reach), FILL, jnp.float32), upper[:-1]], axis=0)
        spilled = jnp.concatenate([spilled, jnp.full((N_TM, segment - reach), FILL, jnp.float32)], axis=1)
        profile_best = jnp.minimum(profile_best, jnp.minimum(owned, spilled).reshape(-1))
    return profile_best
```

```python
import functools

import jax
import jax.numpy as jnp
from jax import lax
from jax.experimental import pallas as pl
from jax.experimental.pallas import tpu as pltpu
from jax.sharding import PartitionSpec as P

M = 256
KB = 32
FILL = 1e30
LANES = 128
SUB = 8
STEP = KB // SUB
WROWS = LANES + KB
XROWS = LANES + KB + M
BIG = 1e30
UNROLL = 8


def shifted(shard, axis, by):
    size = lax.axis_size(axis)
    return lax.ppermute(shard, axis, [(i, (i + by) % size) for i in range(size)])


def swapped(shard, axis, bit):
    size = lax.axis_size(axis)
    return lax.ppermute(shard, axis, [(i, i ^ bit) for i in range(size)])


def group_offsets(own):
    size = lax.axis_size("diag")
    slots = jnp.where(lax.iota(jnp.int32, LANES) == lax.axis_index("diag"), own[0], 0)
    bit = 1
    while bit < size:
        slots = slots + swapped(slots, "diag", bit)
        bit *= 2
    return slots


def split3(x):
    hi = x.astype(jnp.bfloat16)
    rest = x - hi.astype(jnp.float32)
    mid = rest.astype(jnp.bfloat16)
    low = (rest - mid.astype(jnp.float32)).astype(jnp.bfloat16)
    return hi, mid, low


def window_pieces(x, ones):
    out = None
    for piece in split3(x):
        part = jnp.dot(piece, ones, preferred_element_type=jnp.float32)
        out = part if out is None else out + part
    return out


def kernel(geo, offs_ref, excl_ref, left_ref, own_ref, right_ref, tail_ref, out_ref,
           ext, sums, text, stext, utext, xband, sband, uband, pband, xown, mown, best):
    segrows, share_rows, back, nrows, groups, places = geo
    place = lax.axis_index("tm")
    diag = lax.axis_index("diag")
    excl = excl_ref[0]

    ext[0:segrows, :] = left_ref[...]
    ext[segrows : 2 * segrows, :] = own_ref[...]
    last = place == places - 1

    @pl.when(last)
    def _():
        tail_rows = M // LANES
        ext[2 * segrows : 2 * segrows + tail_rows, :] = tail_ref[...]
        ext[2 * segrows + tail_rows : 3 * segrows, :] = jnp.zeros(
            (segrows - tail_rows, LANES), jnp.float32
        )

    @pl.when(jnp.logical_not(last))
    def _():
        ext[2 * segrows : 3 * segrows, :] = right_ref[...]

    if ext.shape[0] > 3 * segrows:
        ext[3 * segrows :, :] = jnp.zeros((ext.shape[0] - 3 * segrows, LANES), jnp.float32)
    first_row = pl.multiple_of(segrows - back + share_rows * diag, SUB)
    x = ext[pl.ds(first_row, 2 * LANES), :]

    rid = lax.broadcasted_iota(jnp.int32, (LANES, 2 * LANES), 0)
    cid = lax.broadcasted_iota(jnp.int32, (LANES, 2 * LANES), 1)
    ones = jnp.where(
        cid < LANES, (rid >= cid).astype(jnp.float32), (rid < cid - LANES).astype(jnp.float32)
    ).astype(jnp.bfloat16)
    held = 2 * LANES - SUB

    def windows(values):
        sums[...] = window_pieces(values, ones)
        return (
            sums[0:held, 0:LANES]
            + (sums[1 : held + 1, 0:LANES] + sums[1 : held + 1, LANES:])
            + sums[2 : held + 2, LANES:]
        )

    mean = windows(x) * (1.0 / M)
    second = windows(x * x) * (1.0 / M)
    spread = lax.rsqrt(second - mean * mean + 1e-05)
    pad = jnp.zeros((SUB, LANES), jnp.float32)

    def turned(values):
        return jnp.concatenate([values[0:LANES].T, values[LANES:].T], axis=1)

    xt = turned(x)
    mt = turned(jnp.concatenate([mean, pad], axis=0))
    st = turned(jnp.concatenate([spread, pad], axis=0))
    ut = mt * st
    st256 = st * (1.0 / M)

    def spread_out(ref, values, turns):
        for tile in range(3):
            for n in range(turns):
                by = (LANES // 2) * tile + n
                moved = pltpu.roll(values, (2 * LANES - by) % (2 * LANES), 1) if by else values
                ref[tile, n * LANES : (n + 1) * LANES, :] = moved[:, 0:LANES]

    spread_out(text, xt, 5)
    spread_out(stext, st256, 3)
    spread_out(utext, ut, 3)

    lane = lax.broadcasted_iota(jnp.int32, (LANES, LANES), 1)

    def own_rows(values, n):
        moved = pltpu.roll(values, (2 * LANES - back - n) % (2 * LANES), 1)[:, 0:LANES]
        width = share_rows
        while width < LANES:
            moved = jnp.where((lane & width) != 0, pltpu.roll(moved, width, 1), moved)
            width *= 2
        return moved

    for n in range(3):
        xown[n * LANES : (n + 1) * LANES, :] = own_rows(xt, n)
    mown[...] = own_rows(mt, 0)
    spread_own = own_rows(st, 0)

    lane8 = lax.broadcasted_iota(jnp.int32, (1, LANES), 1)
    sub8 = lax.broadcasted_iota(jnp.int32, (SUB, LANES), 0)
    limit = places * segrows * LANES
    own_start = (place * segrows + share_rows * diag) * LANES
    lane_row = (lane8 & (share_rows - 1)) * LANES
    hide = []
    for way in range(2):
        first_lag = jnp.zeros((1, LANES), jnp.int32)
        lo = jnp.zeros((1, LANES), jnp.int32)
        xs = ss = us = None
        for g in range(groups):
            off = offs_ref[g]
            lag = off if way == 0 else -(off + (KB - 1))
            base = back * LANES + lag
            col = base // LANES
            row = base - col * LANES
            tile = col // (LANES // 2)
            turn = (share_rows * g - (col - tile * (LANES // 2)) + LANES) % LANES
            here = (lane8 >= share_rows * g) & (lane8 < share_rows * (g + 1))
            first_lag = jnp.where(here, lag, first_lag)

            def merged(ref, rows, acc):
                part = pltpu.roll(ref[tile, pl.ds(row, rows), :], turn, 1)
                return part if acc is None else jnp.where(here, part, acc)

            xs = merged(text, XROWS, xs)
            ss = merged(stext, WROWS, ss)
            us = merged(utext, WROWS, us)
        xband[way] = xs
        sband[way] = ss
        uband[way] = us
        position = (
            own_start + lane_row + first_lag + lax.broadcasted_iota(jnp.int32, (WROWS, LANES), 0)
        )
        pband[way] = jnp.where((position >= 0) & (position < limit), BIG, -BIG)
        for s in range(STEP):
            lag = first_lag + STEP * sub8 + s
            hide.append(jnp.abs(lag) < excl)

    chains = 2 * STEP

    def band(ref, way, start):
        return ref[way, pl.ds(start, SUB, stride=STEP), :]

    def row(ref, i):
        return ref[pl.ds(i, SUB, stride=0), :]

    def first(step, sums_):
        sums_ = list(sums_)
        for u in range(UNROLL):
            i = step * UNROLL + u
            xi = row(xown, i)
            for way in range(2):
                for s in range(STEP):
                    c = way * STEP + s
                    sums_[c] = sums_[c] + xi * band(xband, way, i + s)
        return tuple(sums_)

    zero = jnp.zeros((SUB, LANES), jnp.float32)
    start = lax.fori_loop(0, M // UNROLL, first, (zero,) * chains)
    start = tuple(jnp.where(h, -BIG, q) for h, q in zip(hide, start))

    def advance(step, products):
        products = list(products)
        for u in range(UNROLL):
            i = step * UNROLL + u
            xi = row(xown, i)
            xn = row(xown, i + M)
            mi = row(mown, i)
            top = None
            for way in range(2):
                for s in range(STEP):
                    c = way * STEP + s
                    q = products[c]
                    value = q * band(sband, way, i + s) - mi * band(uband, way, i + s)
                    value = jnp.minimum(value, band(pband, way, i + s))
                    top = value if top is None else jnp.maximum(top, value)
                    products[c] = q + (
                        xn * band(xband, way, i + s + M) - xi * band(xband, way, i + s)
                    )
            best[pl.ds(pl.multiple_of(i * SUB, SUB), SUB), :] = top
        return tuple(products)

    lax.fori_loop(0, LANES // UNROLL, advance, start)

    blocks = []
    for block in range(LANES // SUB):
        top = None
        for h in range(SUB):
            part = best[pl.ds(block * SUB * SUB + h, SUB, stride=SUB), :]
            top = part if top is None else jnp.maximum(top, part)
        blocks.append(top)
    top = jnp.concatenate(blocks, axis=0)
    width = share_rows
    while width < LANES:
        top = jnp.maximum(top, pltpu.roll(top, width, 1))
        width *= 2
    distance = jnp.sqrt(jnp.maximum(1.0 - top * spread_own, 0.0))
    distance = jnp.where(top < -1e20, FILL, distance)
    out_ref[...] = distance.T[0:share_rows, :]


def on_device(series, tail, diag_offsets, exclusion):
    segment = series.shape[0]
    groups = lax.axis_size("diag")
    places = lax.axis_size("tm")
    reach = segment // 2 + segment // 4
    segrows = segment // LANES
    share_rows = segrows // groups
    back = reach // LANES
    deepest = segrows - back + share_rows * (groups - 1)
    geo = (segrows, share_rows, back, 2 * back + share_rows, groups, places)
    left = shifted(series, "tm", 1)
    right = shifted(series, "tm", -1)
    offsets = group_offsets(diag_offsets)
    f32 = jnp.float32
    rows = lambda a: a.reshape(-1, LANES)
    smem = pl.BlockSpec(memory_space=pltpu.SMEM)
    vmem = pl.BlockSpec(memory_space=pltpu.VMEM)
    out = pl.pallas_call(
        functools.partial(kernel, geo),
        out_shape=jax.ShapeDtypeStruct((share_rows, LANES), f32),
        in_specs=[smem, smem, vmem, vmem, vmem, vmem],
        out_specs=vmem,
        scratch_shapes=[
            pltpu.VMEM((max(3 * segrows, deepest + 2 * LANES), LANES), f32),
            pltpu.VMEM((2 * LANES, 2 * LANES), f32),
            pltpu.VMEM((3, 5 * LANES, LANES), f32),
            pltpu.VMEM((3, 3 * LANES, LANES), f32),
            pltpu.VMEM((3, 3 * LANES, LANES), f32),
            pltpu.VMEM((2, XROWS, LANES), f32),
            pltpu.VMEM((2, WROWS, LANES), f32),
            pltpu.VMEM((2, WROWS, LANES), f32),
            pltpu.VMEM((2, WROWS, LANES), f32),
            pltpu.VMEM((3 * LANES, LANES), f32),
            pltpu.VMEM((LANES, LANES), f32),
            pltpu.VMEM((LANES * SUB, LANES), f32),
        ],
    )(offsets, exclusion, rows(left), rows(series), rows(right), rows(tail))
    return out.reshape(-1)


def solution(mesh):
    in_specs = (P("tm"), P(), P("diag"), P())
    out_specs = P(("tm", "diag"))
    return jax.shard_map(
        on_device, mesh=mesh, in_specs=in_specs, out_specs=out_specs, check_vma=False
    )
```

```python
import functools

import jax
import jax.numpy as jnp
from jax import lax
from jax.experimental import pallas as pl
from jax.experimental.pallas import tpu as pltpu
from jax.sharding import PartitionSpec as P

M = 256
KB = 32
FILL = 1e30
LANES = 128
SUB = 8
STEP = KB // SUB
WROWS = LANES + KB
XROWS = LANES + KB + M
BIG = 1e30
UNROLL = 8
VMEM_LIMIT = 16 << 20
COST_A = 1 << 23


def shifted(shard, axis, by):
    size = lax.axis_size(axis)
    return lax.ppermute(shard, axis, [(i, (i + by) % size) for i in range(size)])


def swapped(shard, axis, bit):
    size = lax.axis_size(axis)
    return lax.ppermute(shard, axis, [(i, i ^ bit) for i in range(size)])


def group_offsets(own):
    size = lax.axis_size("diag")
    slots = jnp.where(lax.iota(jnp.int32, LANES) == lax.axis_index("diag"), own[0], 0)
    other = jnp.zeros_like(slots)
    bit = 1
    while bit < size:
        slots = slots + other
        other = swapped(slots, "diag", bit)
        bit *= 2
    return slots, other


def split3(x):
    hi = x.astype(jnp.bfloat16)
    rest = x - hi.astype(jnp.float32)
    mid = rest.astype(jnp.bfloat16)
    low = (rest - mid.astype(jnp.float32)).astype(jnp.bfloat16)
    return hi, mid, low


def window_pieces(x, ones):
    out = None
    for piece in split3(x):
        part = jnp.dot(piece, ones, preferred_element_type=jnp.float32)
        out = part if out is None else out + part
    return out


def prepare(geo, left_ref, own_ref, right_ref, tail_ref,
            text, stext, utext, xown, mown, sown, ext, sums):
    segrows, share_rows, back, groups, places = geo
    place = lax.axis_index("tm")
    diag = lax.axis_index("diag")

    ext[0:segrows, :] = left_ref[...]
    ext[segrows : 2 * segrows, :] = own_ref[...]
    last = place == places - 1

    @pl.when(last)
    def _():
        tail_rows = M // LANES
        ext[2 * segrows : 2 * segrows + tail_rows, :] = tail_ref[...]
        ext[2 * segrows + tail_rows : 3 * segrows, :] = jnp.zeros(
            (segrows - tail_rows, LANES), jnp.float32
        )

    @pl.when(jnp.logical_not(last))
    def _():
        ext[2 * segrows : 3 * segrows, :] = right_ref[...]

    if ext.shape[0] > 3 * segrows:
        ext[3 * segrows :, :] = jnp.zeros((ext.shape[0] - 3 * segrows, LANES), jnp.float32)
    first_row = pl.multiple_of(segrows - back + share_rows * diag, SUB)
    x = ext[pl.ds(first_row, 2 * LANES), :]

    rid = lax.broadcasted_iota(jnp.int32, (LANES, 2 * LANES), 0)
    cid = lax.broadcasted_iota(jnp.int32, (LANES, 2 * LANES), 1)
    ones = jnp.where(
        cid < LANES, (rid >= cid).astype(jnp.float32), (rid < cid - LANES).astype(jnp.float32)
    ).astype(jnp.bfloat16)
    held = 2 * LANES - SUB

    def windows(values):
        sums[...] = window_pieces(values, ones)
        return (
            sums[0:held, 0:LANES]
            + (sums[1 : held + 1, 0:LANES] + sums[1 : held + 1, LANES:])
            + sums[2 : held + 2, LANES:]
        )

    mean = windows(x) * (1.0 / M)
    second = windows(x * x) * (1.0 / M)
    spread = lax.rsqrt(second - mean * mean + 1e-05)
    pad = jnp.zeros((SUB, LANES), jnp.float32)

    def turned(values):
        return jnp.concatenate([values[0:LANES].T, values[LANES:].T], axis=1)

    xt = turned(x)
    mt = turned(jnp.concatenate([mean, pad], axis=0))
    st = turned(jnp.concatenate([spread, pad], axis=0))
    ut = mt * st
    st256 = st * (1.0 / M)

    def spread_out(ref, values, turns):
        for tile in range(3):
            for n in range(turns):
                by = (LANES // 2) * tile + n
                moved = pltpu.roll(values, (2 * LANES - by) % (2 * LANES), 1) if by else values
                ref[tile, n * LANES : (n + 1) * LANES, :] = moved[:, 0:LANES]

    spread_out(text, xt, 5)
    spread_out(stext, st256, 3)
    spread_out(utext, ut, 3)

    lane = lax.broadcasted_iota(jnp.int32, (LANES, LANES), 1)

    def own_rows(values, n):
        moved = pltpu.roll(values, (2 * LANES - back - n) % (2 * LANES), 1)[:, 0:LANES]
        width = share_rows
        while width < LANES:
            moved = jnp.where((lane & width) != 0, pltpu.roll(moved, width, 1), moved)
            width *= 2
        return moved

    for n in range(3):
        xown[n * LANES : (n + 1) * LANES, :] = own_rows(xt, n)
    mown[...] = own_rows(mt, 0)
    sown[...] = own_rows(st, 0)


def profile(geo, mine_ref, other_ref, excl_ref, text, stext, utext, xown, mown, sown, out_ref,
            xband, sband, uband, pband, best):
    segrows, share_rows, back, groups, places = geo
    place = lax.axis_index("tm")
    diag = lax.axis_index("diag")
    excl = excl_ref[0]
    offsets = mine_ref[...] + other_ref[...]

    lane8 = lax.broadcasted_iota(jnp.int32, (1, LANES), 1)
    sub8 = lax.broadcasted_iota(jnp.int32, (SUB, LANES), 0)
    limit = places * segrows * LANES
    own_start = (place * segrows + share_rows * diag) * LANES
    lane_row = (lane8 & (share_rows - 1)) * LANES
    hide = []
    for way in range(2):
        first_lag = jnp.zeros((1, LANES), jnp.int32)
        lo = jnp.zeros((1, LANES), jnp.int32)
        xs = ss = us = None
        for g in range(groups):
            off = offsets[0, g]
            lag = off if way == 0 else -(off + (KB - 1))
            base = back * LANES + lag
            col = base // LANES
            row = base - col * LANES
            tile = col // (LANES // 2)
            turn = (share_rows * g - (col - tile * (LANES // 2)) + LANES) % LANES
            here = (lane8 >= share_rows * g) & (lane8 < share_rows * (g + 1))
            first_lag = jnp.where(here, lag, first_lag)

            def merged(ref, rows, acc):
                part = pltpu.roll(ref[tile, pl.ds(row, rows), :], turn, 1)
                return part if acc is None else jnp.where(here, part, acc)

            xs = merged(text, XROWS, xs)
            ss = merged(stext, WROWS, ss)
            us = merged(utext, WROWS, us)
        xband[way] = xs
        sband[way] = ss
        uband[way] = us
        position = (
            own_start + lane_row + first_lag + lax.broadcasted_iota(jnp.int32, (WROWS, LANES), 0)
        )
        pband[way] = jnp.where((position >= 0) & (position < limit), BIG, -BIG)
        for s in range(STEP):
            lag = first_lag + STEP * sub8 + s
            hide.append(jnp.abs(lag) < excl)

    chains = 2 * STEP

    def band(ref, way, start):
        return ref[way, pl.ds(start, SUB, stride=STEP), :]

    def row(ref, i):
        return ref[pl.ds(i, SUB, stride=0), :]

    def first(step, sums_):
        sums_ = list(sums_)
        for u in range(UNROLL):
            i = step * UNROLL + u
            xi = row(xown, i)
            for way in range(2):
                for s in range(STEP):
                    c = way * STEP + s
                    sums_[c] = sums_[c] + xi * band(xband, way, i + s)
        return tuple(sums_)

    zero = jnp.zeros((SUB, LANES), jnp.float32)
    start = lax.fori_loop(0, M // UNROLL, first, (zero,) * chains)
    start = tuple(jnp.where(h, -BIG, q) for h, q in zip(hide, start))

    def advance(step, products):
        products = list(products)
        for u in range(UNROLL):
            i = step * UNROLL + u
            xi = row(xown, i)
            xn = row(xown, i + M)
            mi = row(mown, i)
            top = None
            for way in range(2):
                for s in range(STEP):
                    c = way * STEP + s
                    q = products[c]
                    value = q * band(sband, way, i + s) - mi * band(uband, way, i + s)
                    value = jnp.minimum(value, band(pband, way, i + s))
                    top = value if top is None else jnp.maximum(top, value)
                    products[c] = q + (
                        xn * band(xband, way, i + s + M) - xi * band(xband, way, i + s)
                    )
            best[pl.ds(pl.multiple_of(i * SUB, SUB), SUB), :] = top
        return tuple(products)

    lax.fori_loop(0, LANES // UNROLL, advance, start)

    blocks = []
    for block in range(LANES // SUB):
        top = None
        for h in range(SUB):
            part = best[pl.ds(block * SUB * SUB + h, SUB, stride=SUB), :]
            top = part if top is None else jnp.maximum(top, part)
        blocks.append(top)
    top = jnp.concatenate(blocks, axis=0)
    width = share_rows
    while width < LANES:
        top = jnp.maximum(top, pltpu.roll(top, width, 1))
        width *= 2
    distance = jnp.sqrt(jnp.maximum(1.0 - top * sown[...], 0.0))
    distance = jnp.where(top < -1e20, FILL, distance)
    out_ref[...] = distance.T[0:share_rows, :]


def on_device(series, tail, diag_offsets, exclusion):
    segment = series.shape[0]
    groups = lax.axis_size("diag")
    places = lax.axis_size("tm")
    reach = segment // 2 + segment // 4
    segrows = segment // LANES
    share_rows = segrows // groups
    back = reach // LANES
    deepest = segrows - back + share_rows * (groups - 1)
    geo = (segrows, share_rows, back, groups, places)
    mine, other = group_offsets(diag_offsets)
    left = shifted(series, "tm", 1)
    right = shifted(series, "tm", -1)
    f32 = jnp.float32
    rows = lambda a: a.reshape(-1, LANES)
    smem = pl.BlockSpec(memory_space=pltpu.SMEM)
    vmem = pl.BlockSpec(memory_space=pltpu.VMEM)
    tables = pl.pallas_call(
        functools.partial(prepare, geo),
        out_shape=[
            jax.ShapeDtypeStruct((3, 5 * LANES, LANES), f32),
            jax.ShapeDtypeStruct((3, 3 * LANES, LANES), f32),
            jax.ShapeDtypeStruct((3, 3 * LANES, LANES), f32),
            jax.ShapeDtypeStruct((3 * LANES, LANES), f32),
            jax.ShapeDtypeStruct((LANES, LANES), f32),
            jax.ShapeDtypeStruct((LANES, LANES), f32),
        ],
        in_specs=[vmem] * 4,
        out_specs=[vmem] * 6,
        scratch_shapes=[
            pltpu.VMEM((max(3 * segrows, deepest + 2 * LANES), LANES), f32),
            pltpu.VMEM((2 * LANES, 2 * LANES), f32),
        ],
        compiler_params=pltpu.CompilerParams(vmem_limit_bytes=VMEM_LIMIT),
        cost_estimate=pl.CostEstimate(flops=COST_A, bytes_accessed=1 << 20, transcendentals=0),
        name="prepare",
    )(rows(left), rows(series), rows(right), rows(tail))
    out = pl.pallas_call(
        functools.partial(profile, geo),
        out_shape=jax.ShapeDtypeStruct((share_rows, LANES), f32),
        in_specs=[vmem, vmem, smem] + [vmem] * 6,
        out_specs=vmem,
        scratch_shapes=[
            pltpu.VMEM((2, XROWS, LANES), f32),
            pltpu.VMEM((2, WROWS, LANES), f32),
            pltpu.VMEM((2, WROWS, LANES), f32),
            pltpu.VMEM((2, WROWS, LANES), f32),
            pltpu.VMEM((LANES * SUB, LANES), f32),
        ],
        compiler_params=pltpu.CompilerParams(vmem_limit_bytes=VMEM_LIMIT),
        cost_estimate=pl.CostEstimate(flops=1 << 24, bytes_accessed=1 << 20, transcendentals=0),
        name="profile",
    )(rows(mine), rows(other), exclusion, *tables)
    return out.reshape(-1)


def solution(mesh):
    in_specs = (P("tm"), P(), P("diag"), P())
    out_specs = P(("tm", "diag"))
    return jax.shard_map(
        on_device, mesh=mesh, in_specs=in_specs, out_specs=out_specs, check_vma=False
    )
```

```python
import functools

import jax
import jax.numpy as jnp
from jax import lax
from jax.experimental import pallas as pl
from jax.experimental.pallas import tpu as pltpu
from jax.sharding import PartitionSpec as P

M = 256
KB = 32
FILL = 1e30
LANES = 128
SUB = 8
STEP = KB // SUB
WROWS = LANES + KB
XROWS = LANES + KB + M
BIG = 1e30
UNROLL = 8
VMEM_LIMIT = 16 << 20
COST_A = 1 << 23
COST_STAGE = 1 << 21


def swapped(shard, axis, partner):
    size = lax.axis_size(axis)
    return lax.ppermute(shard, axis, [(i, partner(i) % size) for i in range(size)])


def group_offsets(own, exclusion):
    size = lax.axis_size("diag")
    lanes = lax.iota(jnp.int32, LANES)
    slots = jnp.where(lanes == lax.axis_index("diag"), own[0], 0)
    other = jnp.zeros_like(slots)
    bit = 1
    while bit < size:
        slots = slots + other
        other = swapped(slots, "diag", lambda i: i ^ bit)
        bit *= 2
    return slots + jnp.where(lanes == LANES - 1, exclusion[0], 0), other


def split3(x):
    hi = x.astype(jnp.bfloat16)
    rest = x - hi.astype(jnp.float32)
    mid = rest.astype(jnp.bfloat16)
    low = (rest - mid.astype(jnp.float32)).astype(jnp.bfloat16)
    return hi, mid, low


def window_pieces(x, ones):
    out = None
    for piece in split3(x):
        part = jnp.dot(piece, ones, preferred_element_type=jnp.float32)
        out = part if out is None else out + part
    return out


def stage(series_ref, tail_ref, series_out, tail_out, sems):
    copies = [
        pltpu.make_async_copy(series_ref, series_out, sems.at[0]),
        pltpu.make_async_copy(tail_ref, tail_out, sems.at[1]),
    ]
    for copy in copies:
        copy.start()
    for copy in copies:
        copy.wait()


def prepare(geo, near_ref, own_ref, far_ref, tail_ref,
            text, stext, utext, xown, mown, sown, ext, sums):
    segrows, share_rows, back, groups, places = geo
    place = lax.axis_index("tm")
    diag = lax.axis_index("diag")

    odd = lax.rem(place, 2) == 1
    last = place == places - 1
    ext[segrows : 2 * segrows, :] = own_ref[...]

    @pl.when(odd)
    def _():
        ext[0:segrows, :] = near_ref[...]
        ext[2 * segrows : 3 * segrows, :] = far_ref[...]

    @pl.when(jnp.logical_not(odd))
    def _():
        ext[0:segrows, :] = far_ref[...]
        ext[2 * segrows : 3 * segrows, :] = near_ref[...]

    @pl.when(last)
    def _():
        tail_rows = M // LANES
        ext[2 * segrows : 2 * segrows + tail_rows, :] = tail_ref[...]
        ext[2 * segrows + tail_rows : 3 * segrows, :] = jnp.zeros(
            (segrows - tail_rows, LANES), jnp.float32
        )

    if ext.shape[0] > 3 * segrows:
        ext[3 * segrows :, :] = jnp.zeros((ext.shape[0] - 3 * segrows, LANES), jnp.float32)
    first_row = pl.multiple_of(segrows - back + share_rows * diag, SUB)
    x = ext[pl.ds(first_row, 2 * LANES), :]

    rid = lax.broadcasted_iota(jnp.int32, (LANES, 2 * LANES), 0)
    cid = lax.broadcasted_iota(jnp.int32, (LANES, 2 * LANES), 1)
    ones = jnp.where(
        cid < LANES, (rid >= cid).astype(jnp.float32), (rid < cid - LANES).astype(jnp.float32)
    ).astype(jnp.bfloat16)
    held = 2 * LANES - SUB

    def windows(values):
        sums[...] = window_pieces(values, ones)
        return (
            sums[0:held, 0:LANES]
            + (sums[1 : held + 1, 0:LANES] + sums[1 : held + 1, LANES:])
            + sums[2 : held + 2, LANES:]
        )

    mean = windows(x) * (1.0 / M)
    second = windows(x * x) * (1.0 / M)
    spread = lax.rsqrt(second - mean * mean + 1e-05)
    pad = jnp.zeros((SUB, LANES), jnp.float32)

    def turned(values):
        return jnp.concatenate([values[0:LANES].T, values[LANES:].T], axis=1)

    xt = turned(x)
    mt = turned(jnp.concatenate([mean, pad], axis=0))
    st = turned(jnp.concatenate([spread, pad], axis=0))
    ut = mt * st
    st256 = st * (1.0 / M)

    def spread_out(ref, values, turns):
        for tile in range(3):
            for n in range(turns):
                by = (LANES // 2) * tile + n
                moved = pltpu.roll(values, (2 * LANES - by) % (2 * LANES), 1) if by else values
                ref[tile, n * LANES : (n + 1) * LANES, :] = moved[:, 0:LANES]

    spread_out(text, xt, 5)
    spread_out(stext, st256, 3)
    spread_out(utext, ut, 3)

    lane = lax.broadcasted_iota(jnp.int32, (LANES, LANES), 1)

    def own_rows(values, n):
        moved = pltpu.roll(values, (2 * LANES - back - n) % (2 * LANES), 1)[:, 0:LANES]
        width = share_rows
        while width < LANES:
            moved = jnp.where((lane & width) != 0, pltpu.roll(moved, width, 1), moved)
            width *= 2
        return moved

    for n in range(3):
        xown[n * LANES : (n + 1) * LANES, :] = own_rows(xt, n)
    mown[...] = own_rows(mt, 0)
    sown[...] = own_rows(st, 0)


def profile(geo, mine_ref, other_ref, text, stext, utext, xown, mown, sown, out_ref,
            xband, sband, uband, pband, best):
    segrows, share_rows, back, groups, places = geo
    place = lax.axis_index("tm")
    diag = lax.axis_index("diag")
    offsets = mine_ref[...] + other_ref[...]
    excl = mine_ref[0, LANES - 1]

    lane8 = lax.broadcasted_iota(jnp.int32, (1, LANES), 1)
    sub8 = lax.broadcasted_iota(jnp.int32, (SUB, LANES), 0)
    limit = places * segrows * LANES
    own_start = (place * segrows + share_rows * diag) * LANES
    lane_row = (lane8 & (share_rows - 1)) * LANES
    hide = []
    for way in range(2):
        first_lag = jnp.zeros((1, LANES), jnp.int32)
        lo = jnp.zeros((1, LANES), jnp.int32)
        xs = ss = us = None
        for g in range(groups):
            off = offsets[0, g]
            lag = off if way == 0 else -(off + (KB - 1))
            base = back * LANES + lag
            col = base // LANES
            row = base - col * LANES
            tile = col // (LANES // 2)
            turn = (share_rows * g - (col - tile * (LANES // 2)) + LANES) % LANES
            here = (lane8 >= share_rows * g) & (lane8 < share_rows * (g + 1))
            first_lag = jnp.where(here, lag, first_lag)

            def merged(ref, rows, acc):
                part = pltpu.roll(ref[tile, pl.ds(row, rows), :], turn, 1)
                return part if acc is None else jnp.where(here, part, acc)

            xs = merged(text, XROWS, xs)
            ss = merged(stext, WROWS, ss)
            us = merged(utext, WROWS, us)
        xband[way] = xs
        sband[way] = ss
        uband[way] = us
        position = (
            own_start + lane_row + first_lag + lax.broadcasted_iota(jnp.int32, (WROWS, LANES), 0)
        )
        pband[way] = jnp.where((position >= 0) & (position < limit), BIG, -BIG)
        for s in range(STEP):
            lag = first_lag + STEP * sub8 + s
            hide.append(jnp.abs(lag) < excl)

    chains = 2 * STEP

    def band(ref, way, start):
        return ref[way, pl.ds(start, SUB, stride=STEP), :]

    def row(ref, i):
        return ref[pl.ds(i, SUB, stride=0), :]

    def first(step, sums_):
        sums_ = list(sums_)
        for u in range(UNROLL):
            i = step * UNROLL + u
            xi = row(xown, i)
            for way in range(2):
                for s in range(STEP):
                    c = way * STEP + s
                    sums_[c] = sums_[c] + xi * band(xband, way, i + s)
        return tuple(sums_)

    zero = jnp.zeros((SUB, LANES), jnp.float32)
    start = lax.fori_loop(0, M // UNROLL, first, (zero,) * chains)
    start = tuple(jnp.where(h, -BIG, q) for h, q in zip(hide, start))

    def advance(step, products):
        products = list(products)
        for u in range(UNROLL):
            i = step * UNROLL + u
            xi = row(xown, i)
            xn = row(xown, i + M)
            mi = row(mown, i)
            top = None
            for way in range(2):
                for s in range(STEP):
                    c = way * STEP + s
                    q = products[c]
                    value = q * band(sband, way, i + s) - mi * band(uband, way, i + s)
                    value = jnp.minimum(value, band(pband, way, i + s))
                    top = value if top is None else jnp.maximum(top, value)
                    products[c] = q + (
                        xn * band(xband, way, i + s + M) - xi * band(xband, way, i + s)
                    )
            best[pl.ds(pl.multiple_of(i * SUB, SUB), SUB), :] = top
        return tuple(products)

    lax.fori_loop(0, LANES // UNROLL, advance, start)

    blocks = []
    for block in range(LANES // SUB):
        top = None
        for h in range(SUB):
            part = best[pl.ds(block * SUB * SUB + h, SUB, stride=SUB), :]
            top = part if top is None else jnp.maximum(top, part)
        blocks.append(top)
    top = jnp.concatenate(blocks, axis=0)
    width = share_rows
    while width < LANES:
        top = jnp.maximum(top, pltpu.roll(top, width, 1))
        width *= 2
    distance = jnp.sqrt(jnp.maximum(1.0 - top * sown[...], 0.0))
    distance = jnp.where(top < -1e20, FILL, distance)
    out_ref[...] = distance.T[0:share_rows, :]


def on_device(series, tail, diag_offsets, exclusion):
    segment = series.shape[0]
    groups = lax.axis_size("diag")
    places = lax.axis_size("tm")
    reach = segment // 2 + segment // 4
    segrows = segment // LANES
    share_rows = segrows // groups
    back = reach // LANES
    deepest = segrows - back + share_rows * (groups - 1)
    geo = (segrows, share_rows, back, groups, places)
    f32 = jnp.float32
    rows = lambda a: a.reshape(-1, LANES)
    held = lambda a: pltpu.with_memory_space_constraint(a, pltpu.HBM)
    vmem = pl.BlockSpec(memory_space=pltpu.VMEM)
    hbm = pl.BlockSpec(memory_space=pltpu.HBM)
    mine, other = group_offsets(diag_offsets, exclusion)
    own, end = pl.pallas_call(
        stage,
        out_shape=[
            jax.ShapeDtypeStruct((segrows, LANES), f32),
            jax.ShapeDtypeStruct((M // LANES, LANES), f32),
        ],
        in_specs=[hbm] * 2,
        out_specs=[vmem] * 2,
        scratch_shapes=[pltpu.SemaphoreType.DMA((2,))],
        compiler_params=pltpu.CompilerParams(vmem_limit_bytes=VMEM_LIMIT),
        cost_estimate=pl.CostEstimate(flops=COST_STAGE, bytes_accessed=1 << 17, transcendentals=0),
        name="stage",
    )(held(rows(series)), held(rows(tail)))
    far = swapped(own, "tm", lambda i: i + 1 if i % 2 else i - 1)
    near = swapped(own, "tm", lambda i: i ^ 1)
    tables = pl.pallas_call(
        functools.partial(prepare, geo),
        out_shape=[
            jax.ShapeDtypeStruct((3, 5 * LANES, LANES), f32),
            jax.ShapeDtypeStruct((3, 3 * LANES, LANES), f32),
            jax.ShapeDtypeStruct((3, 3 * LANES, LANES), f32),
            jax.ShapeDtypeStruct((3 * LANES, LANES), f32),
            jax.ShapeDtypeStruct((LANES, LANES), f32),
            jax.ShapeDtypeStruct((LANES, LANES), f32),
        ],
        in_specs=[vmem] * 4,
        out_specs=[vmem] * 6,
        scratch_shapes=[
            pltpu.VMEM((max(3 * segrows, deepest + 2 * LANES), LANES), f32),
            pltpu.VMEM((2 * LANES, 2 * LANES), f32),
        ],
        compiler_params=pltpu.CompilerParams(vmem_limit_bytes=VMEM_LIMIT),
        cost_estimate=pl.CostEstimate(flops=COST_A, bytes_accessed=1 << 20, transcendentals=0),
        name="prepare",
    )(near, own, far, end)
    out = pl.pallas_call(
        functools.partial(profile, geo),
        out_shape=jax.ShapeDtypeStruct((share_rows, LANES), f32),
        in_specs=[vmem] * 8,
        out_specs=vmem,
        scratch_shapes=[
            pltpu.VMEM((2, XROWS, LANES), f32),
            pltpu.VMEM((2, WROWS, LANES), f32),
            pltpu.VMEM((2, WROWS, LANES), f32),
            pltpu.VMEM((2, WROWS, LANES), f32),
            pltpu.VMEM((LANES * SUB, LANES), f32),
        ],
        compiler_params=pltpu.CompilerParams(vmem_limit_bytes=VMEM_LIMIT),
        cost_estimate=pl.CostEstimate(flops=1 << 24, bytes_accessed=1 << 20, transcendentals=0),
        name="profile",
    )(rows(mine), rows(other), *tables)
    return out.reshape(-1)


def solution(mesh):
    in_specs = (P("tm"), P(), P("diag"), P())
    out_specs = P(("tm", "diag"))
    return jax.shard_map(
        on_device, mesh=mesh, in_specs=in_specs, out_specs=out_specs, check_vma=False
    )
```

```python
import functools

import jax
import jax.numpy as jnp
from jax import lax
from jax.experimental import pallas as pl
from jax.experimental.pallas import tpu as pltpu
from jax.sharding import PartitionSpec as P

M = 256
KB = 32
FILL = 1e30
LANES = 128
SUB = 8
STEP = KB // SUB
BROWS = M + KB
BIG = 1e30
UNROLL = 8
VMEM_LIMIT = 16 << 20
COST_A = 1 << 23
COST_STAGE = 1 << 21


def swapped(shard, axis, partner):
    size = lax.axis_size(axis)
    return lax.ppermute(shard, axis, [(i, partner(i) % size) for i in range(size)])


def group_offsets(own, exclusion):
    size = lax.axis_size("diag")
    lanes = lax.iota(jnp.int32, LANES)
    slots = jnp.where(lanes == lax.axis_index("diag"), own[0], 0)
    other = jnp.zeros_like(slots)
    bit = 1
    while bit < size:
        slots = slots + other
        other = swapped(slots, "diag", lambda i: i ^ bit)
        bit *= 2
    return slots + jnp.where(lanes == LANES - 1, exclusion[0], 0), other


def split3(x):
    hi = x.astype(jnp.bfloat16)
    rest = x - hi.astype(jnp.float32)
    mid = rest.astype(jnp.bfloat16)
    low = (rest - mid.astype(jnp.float32)).astype(jnp.bfloat16)
    return hi, mid, low


def window_pieces(x, ones):
    out = None
    for piece in split3(x):
        part = jnp.dot(piece, ones, preferred_element_type=jnp.float32)
        out = part if out is None else out + part
    return out


def stage(series_ref, tail_ref, series_out, tail_out, sems):
    copies = [
        pltpu.make_async_copy(series_ref, series_out, sems.at[0]),
        pltpu.make_async_copy(tail_ref, tail_out, sems.at[1]),
    ]
    for copy in copies:
        copy.start()
    for copy in copies:
        copy.wait()


def prepare(geo, near_ref, own_ref, far_ref, tail_ref,
            points, fall, rise, spreads, own_points, own_fall, own_rise, ext, sums):
    segrows, share_rows, back, groups, places = geo
    place = lax.axis_index("tm")
    diag = lax.axis_index("diag")

    odd = lax.rem(place, 2) == 1
    last = place == places - 1
    ext[segrows : 2 * segrows, :] = own_ref[...]

    @pl.when(odd)
    def _():
        ext[0:segrows, :] = near_ref[...]
        ext[2 * segrows : 3 * segrows, :] = far_ref[...]

    @pl.when(jnp.logical_not(odd))
    def _():
        ext[0:segrows, :] = far_ref[...]
        ext[2 * segrows : 3 * segrows, :] = near_ref[...]

    @pl.when(last)
    def _():
        tail_rows = M // LANES
        ext[2 * segrows : 2 * segrows + tail_rows, :] = tail_ref[...]
        ext[2 * segrows + tail_rows : 3 * segrows, :] = jnp.zeros(
            (segrows - tail_rows, LANES), jnp.float32
        )

    if ext.shape[0] > 3 * segrows:
        ext[3 * segrows :, :] = jnp.zeros((ext.shape[0] - 3 * segrows, LANES), jnp.float32)
    first_row = pl.multiple_of(segrows - back + share_rows * diag, SUB)
    points[...] = ext[pl.ds(first_row, 2 * LANES), :]

    rid = lax.broadcasted_iota(jnp.int32, (LANES, 2 * LANES), 0)
    cid = lax.broadcasted_iota(jnp.int32, (LANES, 2 * LANES), 1)
    ones = jnp.where(
        cid < LANES, (rid >= cid).astype(jnp.float32), (rid < cid - LANES).astype(jnp.float32)
    ).astype(jnp.bfloat16)
    held = 2 * LANES - SUB

    def windows(values):
        sums[...] = window_pieces(values, ones)
        return (
            sums[0:held, 0:LANES]
            + (sums[1 : held + 1, 0:LANES] + sums[1 : held + 1, LANES:])
            + sums[2 : held + 2, LANES:]
        )

    x = points[...]
    mean = windows(x) * (1.0 / M)
    second = windows(x * x) * (1.0 / M)
    here = points[0:held, :]
    there = points[2 : held + 2, :]
    change = there - here
    pad = jnp.zeros((SUB, LANES), jnp.float32)
    spreads[0:held, :] = lax.rsqrt(second - mean * mean + 1e-05)
    fall[0:held, :] = 0.5 * change
    rise[0:held, :] = (there + here) - 2.0 * mean - change * (1.0 / M)
    for ref in (spreads, fall, rise):
        ref[held:, :] = pad

    chunks = share_rows // 2

    def own_rows(ref):
        halves = []
        for half in range(2):
            rows = ref[pl.ds(back + half, chunks, stride=2), :]
            halves.append(jnp.concatenate([rows] * (LANES // chunks), axis=0).T)
        return jnp.concatenate(halves, axis=0)

    turned = own_rows(points)
    own_points[...] = turned - jnp.sum(turned, axis=0, keepdims=True) * (1.0 / M)
    own_fall[...] = own_rows(fall)
    own_rise[...] = own_rows(rise)


def profile(geo, mine_ref, other_ref, points, fall, rise, spreads, own_points, own_fall, own_rise,
            out_ref, moved, xband, fband, rband, sband, pband, best):
    segrows, share_rows, back, groups, places = geo
    place = lax.axis_index("tm")
    diag = lax.axis_index("diag")
    offsets = mine_ref[...] + other_ref[...]
    excl = mine_ref[0, LANES - 1]
    chunks = share_rows // 2

    lane = lax.broadcasted_iota(jnp.int32, (1, LANES), 1)
    sub = lax.broadcasted_iota(jnp.int32, (SUB, LANES), 0)
    lags, bases = [], []
    for way in range(2):
        for g in range(groups):
            off = offsets[0, g]
            lags.append(off if way == 0 else -(off + (KB - 1)))
    first_lag = jnp.zeros((1, LANES), jnp.int32)
    for j, lag in enumerate(lags):
        first_lag = jnp.where(lane >= chunks * j, lag, first_lag)
    rows = moved.shape[1]
    for ref, out in ((points, xband), (spreads, sband), (fall, fband), (rise, rband)):
        parts = [[] for _ in range(3)]
        for j, lag in enumerate(lags):
            base = back * LANES + lag
            row = base // LANES
            inner = base - row * LANES
            turn = lax.rem(LANES - inner, LANES)
            moved[j] = pltpu.roll(ref[pl.ds(row, rows), :], turn, 1)
            near = lane < LANES - inner
            for q in range(3):
                parts[q].append(
                    jnp.where(
                        near,
                        moved[j, pl.ds(q, chunks, stride=2), :],
                        moved[j, pl.ds(q + 1, chunks, stride=2), :],
                    )
                )
        for q in range(3):
            turned = jnp.concatenate(parts[q], axis=0).T
            out[q * LANES : min((q + 1) * LANES, BROWS), :] = turned[0 : min(LANES, BROWS - q * LANES)]
    limit = places * segrows * LANES
    own_start = (place * segrows + share_rows * diag) * LANES
    position = own_start + (lane & (chunks - 1)) * M + first_lag
    position = position + lax.broadcasted_iota(jnp.int32, (BROWS, LANES), 0)
    pband[...] = jnp.where((position >= 0) & (position < limit), BIG, -BIG)

    def band(ref, start):
        return ref[pl.ds(start, SUB, stride=STEP), :]

    def row(ref, i):
        return ref[pl.ds(i, SUB, stride=0), :]

    def first(step, totals):
        totals = list(totals)
        for u in range(UNROLL):
            i = step * UNROLL + u
            xi = row(own_points, i)
            for s in range(STEP):
                c = s + STEP * (u % 2)
                totals[c] = totals[c] + xi * band(xband, i + s)
        return tuple(totals)

    zero = jnp.zeros((SUB, LANES), jnp.float32)
    totals = lax.fori_loop(0, M // UNROLL, first, (zero,) * (2 * STEP))
    start = tuple(
        jnp.where(
            jnp.abs(first_lag + STEP * sub + s) < excl, -BIG, totals[s] + totals[s + STEP]
        )
        for s in range(STEP)
    )

    def advance(step, covs):
        covs = list(covs)
        for u in range(UNROLL):
            i = step * UNROLL + u
            fi = row(own_fall, i)
            ri = row(own_rise, i)
            top = None
            for s in range(STEP):
                value = jnp.minimum(covs[s] * band(sband, i + s), band(pband, i + s))
                top = value if top is None else jnp.maximum(top, value)
                covs[s] = covs[s] + (fi * band(rband, i + s) + ri * band(fband, i + s))
            best[pl.ds(pl.multiple_of(i * SUB, SUB), SUB), :] = top
        return tuple(covs)

    lax.fori_loop(0, M // UNROLL, advance, start)

    for half in range(2):
        blocks = []
        for block in range(LANES // SUB):
            top = None
            for h in range(SUB):
                at = (half * LANES + block * SUB) * SUB + h
                part = best[pl.ds(at, SUB, stride=SUB), :]
                top = part if top is None else jnp.maximum(top, part)
            blocks.append(top)
        turned = jnp.concatenate(blocks, axis=0).T
        top = turned[0:chunks]
        for j in range(1, 2 * groups):
            top = jnp.maximum(top, turned[chunks * j : chunks * (j + 1)])
        spread = spreads[pl.ds(back + half, chunks, stride=2), :]
        distance = jnp.sqrt(jnp.maximum(1.0 - top * (spread * (1.0 / M)), 0.0))
        out_ref[pl.ds(half, chunks, stride=2), :] = jnp.where(top < -1e20, FILL, distance)


def on_device(series, tail, diag_offsets, exclusion):
    segment = series.shape[0]
    groups = lax.axis_size("diag")
    places = lax.axis_size("tm")
    reach = segment // 2 + segment // 4
    segrows = segment // LANES
    share_rows = segrows // groups
    back = reach // LANES
    deepest = segrows - back + share_rows * (groups - 1)
    geo = (segrows, share_rows, back, groups, places)
    f32 = jnp.float32
    rows = lambda a: a.reshape(-1, LANES)
    held = lambda a: pltpu.with_memory_space_constraint(a, pltpu.HBM)
    vmem = pl.BlockSpec(memory_space=pltpu.VMEM)
    hbm = pl.BlockSpec(memory_space=pltpu.HBM)
    mine, other = group_offsets(diag_offsets, exclusion)
    own, end = pl.pallas_call(
        stage,
        out_shape=[
            jax.ShapeDtypeStruct((segrows, LANES), f32),
            jax.ShapeDtypeStruct((M // LANES, LANES), f32),
        ],
        in_specs=[hbm] * 2,
        out_specs=[vmem] * 2,
        scratch_shapes=[pltpu.SemaphoreType.DMA((2,))],
        compiler_params=pltpu.CompilerParams(vmem_limit_bytes=VMEM_LIMIT),
        cost_estimate=pl.CostEstimate(flops=COST_STAGE, bytes_accessed=1 << 17, transcendentals=0),
        name="stage",
    )(held(rows(series)), held(rows(tail)))
    far = swapped(own, "tm", lambda i: i + 1 if i % 2 else i - 1)
    near = swapped(own, "tm", lambda i: i ^ 1)
    table = jax.ShapeDtypeStruct((2 * LANES, LANES), f32)
    tables = pl.pallas_call(
        functools.partial(prepare, geo),
        out_shape=[table] * 7,
        in_specs=[vmem] * 4,
        out_specs=[vmem] * 7,
        scratch_shapes=[
            pltpu.VMEM((max(3 * segrows, deepest + 2 * LANES), LANES), f32),
            pltpu.VMEM((2 * LANES, 2 * LANES), f32),
        ],
        compiler_params=pltpu.CompilerParams(vmem_limit_bytes=VMEM_LIMIT),
        cost_estimate=pl.CostEstimate(flops=COST_A, bytes_accessed=1 << 20, transcendentals=0),
        name="prepare",
    )(near, own, far, end)
    band = pltpu.VMEM((BROWS, LANES), f32)
    out = pl.pallas_call(
        functools.partial(profile, geo),
        out_shape=jax.ShapeDtypeStruct((share_rows, LANES), f32),
        in_specs=[vmem] * 9,
        out_specs=vmem,
        scratch_shapes=[
            pltpu.VMEM((2 * groups, -(-(share_rows + 3) // SUB) * SUB, LANES), f32),
            band,
            band,
            band,
            band,
            band,
            pltpu.VMEM((M * SUB, LANES), f32),
        ],
        compiler_params=pltpu.CompilerParams(vmem_limit_bytes=VMEM_LIMIT),
        cost_estimate=pl.CostEstimate(flops=1 << 24, bytes_accessed=1 << 20, transcendentals=0),
        name="profile",
    )(rows(mine), rows(other), *tables)
    return out.reshape(-1)


def solution(mesh):
    in_specs = (P("tm"), P(), P("diag"), P())
    out_specs = P(("tm", "diag"))
    return jax.shard_map(
        on_device, mesh=mesh, in_specs=in_specs, out_specs=out_specs, check_vma=False
    )
```

```python
import functools

import jax
import jax.numpy as jnp
from jax import lax
from jax.experimental import pallas as pl
from jax.experimental.pallas import tpu as pltpu
from jax.sharding import PartitionSpec as P

M = 256
KB = 32
FILL = 1e30
LANES = 128
SUB = 8
HALF = KB // 2
STEP = HALF // SUB
BROWS = M + HALF
SPAN = M + 4
BIG = 1e30
UNROLL = 64
TOTALS = 4
VMEM_LIMIT = 16 << 20
COST_A = 1 << 23
COST_STAGE = 1 << 21


def swapped(shard, axis, partner):
    size = lax.axis_size(axis)
    return lax.ppermute(shard, axis, [(i, partner(i) % size) for i in range(size)])


def group_offsets(own, exclusion):
    size = lax.axis_size("diag")
    lanes = lax.iota(jnp.int32, LANES)
    slots = jnp.where(lanes == lax.axis_index("diag"), own[0], 0)
    other = jnp.zeros_like(slots)
    bit = 1
    while bit < size:
        slots = slots + other
        other = swapped(slots, "diag", lambda i: i ^ bit)
        bit *= 2
    return slots + jnp.where(lanes == LANES - 1, exclusion[0], 0), other


def split3(x):
    hi = x.astype(jnp.bfloat16)
    rest = x - hi.astype(jnp.float32)
    mid = rest.astype(jnp.bfloat16)
    low = (rest - mid.astype(jnp.float32)).astype(jnp.bfloat16)
    return hi, mid, low


def window_pieces(x, ones):
    out = None
    for piece in split3(x):
        part = jnp.dot(piece, ones, preferred_element_type=jnp.float32)
        out = part if out is None else out + part
    return out


def stage(series_ref, tail_ref, series_out, tail_out, sems):
    copies = [
        pltpu.make_async_copy(series_ref, series_out, sems.at[0]),
        pltpu.make_async_copy(tail_ref, tail_out, sems.at[1]),
    ]
    for copy in copies:
        copy.start()
    for copy in copies:
        copy.wait()


def prepare(geo, near_ref, own_ref, far_ref, tail_ref,
            points, fall, rise, spreads, own_points, own_fall, own_rise, ext, sums):
    segrows, share_rows, back, groups, places = geo
    place = lax.axis_index("tm")
    diag = lax.axis_index("diag")

    odd = lax.rem(place, 2) == 1
    last = place == places - 1
    ext[segrows : 2 * segrows, :] = own_ref[...]

    @pl.when(odd)
    def _():
        ext[0:segrows, :] = near_ref[...]
        ext[2 * segrows : 3 * segrows, :] = far_ref[...]

    @pl.when(jnp.logical_not(odd))
    def _():
        ext[0:segrows, :] = far_ref[...]
        ext[2 * segrows : 3 * segrows, :] = near_ref[...]

    @pl.when(last)
    def _():
        tail_rows = M // LANES
        ext[2 * segrows : 2 * segrows + tail_rows, :] = tail_ref[...]
        ext[2 * segrows + tail_rows : 3 * segrows, :] = jnp.zeros(
            (segrows - tail_rows, LANES), jnp.float32
        )

    if ext.shape[0] > 3 * segrows:
        ext[3 * segrows :, :] = jnp.zeros((ext.shape[0] - 3 * segrows, LANES), jnp.float32)
    first_row = pl.multiple_of(segrows - back + share_rows * diag, SUB)
    points[...] = ext[pl.ds(first_row, 2 * LANES), :]

    rid = lax.broadcasted_iota(jnp.int32, (LANES, 2 * LANES), 0)
    cid = lax.broadcasted_iota(jnp.int32, (LANES, 2 * LANES), 1)
    ones = jnp.where(
        cid < LANES, (rid >= cid).astype(jnp.float32), (rid < cid - LANES).astype(jnp.float32)
    ).astype(jnp.bfloat16)
    held = 2 * LANES - SUB

    def windows(values):
        sums[...] = window_pieces(values, ones)
        return (
            sums[0:held, 0:LANES]
            + (sums[1 : held + 1, 0:LANES] + sums[1 : held + 1, LANES:])
            + sums[2 : held + 2, LANES:]
        )

    x = points[...]
    mean = windows(x) * (1.0 / M)
    second = windows(x * x) * (1.0 / M)
    here = points[0:held, :]
    there = points[2 : held + 2, :]
    change = there - here
    pad = jnp.zeros((SUB, LANES), jnp.float32)
    spreads[0:held, :] = lax.rsqrt(second - mean * mean + 1e-05)
    fall[0:held, :] = 0.5 * change
    rise[0:held, :] = (there + here) - 2.0 * mean - change * (1.0 / M)
    for ref in (spreads, fall, rise):
        ref[held:, :] = pad

    chunks = share_rows // 2

    def own_rows(ref):
        halves = []
        for half in range(2):
            rows = ref[pl.ds(back + half, chunks, stride=2), :]
            halves.append(jnp.concatenate([rows] * (LANES // chunks), axis=0).T)
        return jnp.concatenate(halves, axis=0)

    turned = own_rows(points)
    own_points[...] = turned - jnp.sum(turned, axis=0, keepdims=True) * (1.0 / M)
    own_fall[...] = own_rows(fall)
    own_rise[...] = own_rows(rise)


def sweep(geo, offsets, excl, tables, scratch, before, best):
    points, fall, rise, spreads, own_points, own_fall, own_rise = tables
    moved, xband, fband, rband, sband, pband = scratch
    segrows, share_rows, back, groups, places = geo
    place = lax.axis_index("tm")
    diag = lax.axis_index("diag")
    chunks = share_rows // 2

    lane = lax.broadcasted_iota(jnp.int32, (1, LANES), 1)
    sub = lax.broadcasted_iota(jnp.int32, (SUB, LANES), 0)
    lags = []
    for off in offsets:
        for lag in (off, -(off + (KB - 1))):
            lags += [lag, lag + HALF]
    first_lag = jnp.zeros((1, LANES), jnp.int32)
    for j, lag in enumerate(lags):
        first_lag = jnp.where(lane >= chunks * j, lag, first_lag)
    rows = moved.shape[1]
    def fill(ref, out):
        parts = [[] for _ in range(3)]
        for j, lag in enumerate(lags):
            base = back * LANES + lag
            row = base // LANES
            inner = base - row * LANES
            turn = lax.rem(LANES - inner, LANES)
            moved[j] = pltpu.roll(ref[pl.ds(row, rows), :], turn, 1)
            near = lane < LANES - inner
            for q in range(3):
                parts[q].append(
                    jnp.where(
                        near,
                        moved[j, pl.ds(q, chunks, stride=2), :],
                        moved[j, pl.ds(q + 1, chunks, stride=2), :],
                    )
                )
        for q in range(3):
            held = min(LANES, BROWS - q * LANES)
            turned = jnp.concatenate(parts[q], axis=0).T
            out[q * LANES : q * LANES + held, :] = turned[0:held]

    def band(ref, start):
        return ref[pl.ds(start, SUB, stride=STEP), :]

    def row(ref, i):
        return ref[pl.ds(i, SUB, stride=0), :]

    fill(points, xband)
    totals = [None] * (TOTALS * STEP)
    for i in range(M):
        xi = row(own_points, i)
        for s in range(STEP):
            c = s + STEP * (i % TOTALS)
            term = xi * band(xband, i + s)
            totals[c] = term if totals[c] is None else totals[c] + term
    start = []
    for s in range(STEP):
        parts = list(totals[s::STEP])
        while len(parts) > 1:
            parts = [a + b for a, b in zip(parts[0::2], parts[1::2])]
        start.append(jnp.where(jnp.abs(first_lag + STEP * sub + s) < excl, -BIG, parts[0]))
    fill(spreads, sband)
    fill(fall, fband)
    fill(rise, rband)
    limit = places * segrows * LANES
    own_start = (place * segrows + share_rows * diag) * LANES
    position = own_start + (lane & (chunks - 1)) * M + first_lag
    position = position + lax.broadcasted_iota(jnp.int32, (BROWS, LANES), 0)
    pband[...] = jnp.where((position >= 0) & (position < limit), BIG, -BIG)

    def advance(step, covs):
        covs = list(covs)
        for u in range(UNROLL):
            i = step * UNROLL + u
            fi = row(own_fall, i)
            ri = row(own_rise, i)
            top = None if before is None else before[pl.ds(i, SUB, stride=SPAN), :]
            for s in range(STEP):
                value = jnp.minimum(covs[s] * band(sband, i + s), band(pband, i + s))
                top = value if top is None else jnp.maximum(top, value)
                covs[s] = covs[s] + (fi * band(rband, i + s) + ri * band(fband, i + s))
            best[pl.ds(i, SUB, stride=SPAN), :] = top
        return tuple(covs)

    lax.fori_loop(0, M // UNROLL, advance, tuple(start))


def picked(slots, groups):
    half = groups // 2
    return [slots[0, e] + slots[0, half + e] for e in range(half)]


def early(geo, mine_ref, *refs):
    tables, best, scratch = refs[:7], refs[7], refs[8:]
    slots = mine_ref[...]
    sweep(geo, picked(slots, geo[3]), slots[0, LANES - 1], tables, scratch, None, best)


def late(geo, mine_ref, other_ref, before, *refs):
    tables, out_ref, best, scratch = refs[:7], refs[7], refs[8], refs[9:]
    segrows, share_rows, back, groups, places = geo
    chunks = share_rows // 2
    excl = mine_ref[0, LANES - 1]
    sweep(geo, picked(other_ref[...], groups), excl, tables, scratch, before, best)
    spreads = tables[3]

    for half in range(2):
        blocks = []
        for block in range(LANES // SUB):
            top = None
            for h in range(SUB):
                at = h * SPAN + half * LANES + block * SUB
                part = best[at : at + SUB, :]
                top = part if top is None else jnp.maximum(top, part)
            blocks.append(top)
        turned = jnp.concatenate(blocks, axis=0).T
        top = turned[0:chunks]
        for j in range(1, 2 * groups):
            top = jnp.maximum(top, turned[chunks * j : chunks * (j + 1)])
        spread = spreads[pl.ds(back + half, chunks, stride=2), :]
        distance = jnp.sqrt(jnp.maximum(1.0 - top * (spread * (1.0 / M)), 0.0))
        out_ref[pl.ds(half, chunks, stride=2), :] = jnp.where(top < -1e20, FILL, distance)


def on_device(series, tail, diag_offsets, exclusion):
    segment = series.shape[0]
    groups = lax.axis_size("diag")
    places = lax.axis_size("tm")
    reach = segment // 2 + segment // 4
    segrows = segment // LANES
    share_rows = segrows // groups
    back = reach // LANES
    deepest = segrows - back + share_rows * (groups - 1)
    geo = (segrows, share_rows, back, groups, places)
    f32 = jnp.float32
    rows = lambda a: a.reshape(-1, LANES)
    held = lambda a: pltpu.with_memory_space_constraint(a, pltpu.HBM)
    vmem = pl.BlockSpec(memory_space=pltpu.VMEM)
    hbm = pl.BlockSpec(memory_space=pltpu.HBM)
    mine, other = group_offsets(diag_offsets, exclusion)
    own, end = pl.pallas_call(
        stage,
        out_shape=[
            jax.ShapeDtypeStruct((segrows, LANES), f32),
            jax.ShapeDtypeStruct((M // LANES, LANES), f32),
        ],
        in_specs=[hbm] * 2,
        out_specs=[vmem] * 2,
        scratch_shapes=[pltpu.SemaphoreType.DMA((2,))],
        compiler_params=pltpu.CompilerParams(vmem_limit_bytes=VMEM_LIMIT),
        cost_estimate=pl.CostEstimate(flops=COST_STAGE, bytes_accessed=1 << 17, transcendentals=0),
        name="stage",
    )(held(rows(series)), held(rows(tail)))
    far = swapped(own, "tm", lambda i: i + 1 if i % 2 else i - 1)
    near = swapped(own, "tm", lambda i: i ^ 1)
    table = jax.ShapeDtypeStruct((2 * LANES, LANES), f32)
    tables = pl.pallas_call(
        functools.partial(prepare, geo),
        out_shape=[table] * 7,
        in_specs=[vmem] * 4,
        out_specs=[vmem] * 7,
        scratch_shapes=[
            pltpu.VMEM((max(3 * segrows, deepest + 2 * LANES), LANES), f32),
            pltpu.VMEM((2 * LANES, 2 * LANES), f32),
        ],
        compiler_params=pltpu.CompilerParams(vmem_limit_bytes=VMEM_LIMIT),
        cost_estimate=pl.CostEstimate(flops=COST_A, bytes_accessed=1 << 20, transcendentals=0),
        name="prepare",
    )(near, own, far, end)
    band = pltpu.VMEM((BROWS, LANES), f32)
    moved = pltpu.VMEM((2 * groups, -(-(share_rows + 3) // SUB) * SUB, LANES), f32)
    scratch = [moved, band, band, band, band, band]
    params = pltpu.CompilerParams(vmem_limit_bytes=VMEM_LIMIT)
    maxima = pl.pallas_call(
        functools.partial(early, geo),
        out_shape=jax.ShapeDtypeStruct((SUB * SPAN, LANES), f32),
        in_specs=[vmem] * 8,
        out_specs=vmem,
        scratch_shapes=scratch,
        compiler_params=params,
        cost_estimate=pl.CostEstimate(flops=COST_A, bytes_accessed=1 << 20, transcendentals=0),
        name="early",
    )(rows(mine), *tables)
    out = pl.pallas_call(
        functools.partial(late, geo),
        out_shape=jax.ShapeDtypeStruct((share_rows, LANES), f32),
        in_specs=[vmem] * 10,
        out_specs=vmem,
        scratch_shapes=[pltpu.VMEM((SUB * SPAN, LANES), f32)] + scratch,
        compiler_params=params,
        cost_estimate=pl.CostEstimate(flops=1 << 24, bytes_accessed=1 << 20, transcendentals=0),
        name="late",
    )(rows(mine), rows(other), maxima, *tables)
    return out.reshape(-1)


def solution(mesh):
    in_specs = (P("tm"), P(), P("diag"), P())
    out_specs = P(("tm", "diag"))
    return jax.shard_map(
        on_device, mesh=mesh, in_specs=in_specs, out_specs=out_specs, check_vma=False
    )
```

```python
import functools

import jax
import jax.numpy as jnp
from jax import lax
from jax.experimental import pallas as pl
from jax.experimental.pallas import tpu as pltpu
from jax.sharding import PartitionSpec as P


M = 256
KB = 32
FILL = 1e30
LANES = 128
LANE_BITS = 7
SUB = 8
HALF = KB // 2
STEP = HALF // SUB
BROWS = M + HALF
SPAN = M + 4
BIG = 1e30
UNROLL = 64
TOTALS = 4
VMEM_LIMIT = 16 << 20
COST_A = 1 << 23
COST_LOW = 1 << 30


def swapped(shard, axis, partner):
    size = lax.axis_size(axis)
    return lax.ppermute(shard, axis, [(i, partner(i) % size) for i in range(size)])


def group_offsets(own, exclusion):
    size = lax.axis_size("diag")
    lanes = lax.iota(jnp.int32, LANES)
    slots = jnp.where(lanes == lax.axis_index("diag"), own[0], 0)
    other = jnp.zeros_like(slots)
    bit = 1
    while bit < size:
        slots = slots + other
        other = swapped(slots, "diag", lambda i: i ^ bit)
        bit *= 2
    return slots + jnp.where(lanes == LANES - 1, exclusion[0], 0), other


def split3(x):
    hi = x.astype(jnp.bfloat16)
    rest = x - hi.astype(jnp.float32)
    mid = rest.astype(jnp.bfloat16)
    low = (rest - mid.astype(jnp.float32)).astype(jnp.bfloat16)
    return hi, mid, low


def window_pieces(x, ones):
    out = None
    for piece in split3(x):
        part = jnp.dot(piece, ones, preferred_element_type=jnp.float32)
        out = part if out is None else out + part
    return out


def triangles(ones):
    rid = lax.broadcasted_iota(jnp.int32, (LANES, 2 * LANES), 0)
    cid = lax.broadcasted_iota(jnp.int32, (LANES, 2 * LANES), 1)
    ones[...] = jnp.where(
        cid < LANES, (rid >= cid).astype(jnp.float32), (rid < cid - LANES).astype(jnp.float32)
    ).astype(jnp.bfloat16)


def prepare(geo, near_ref, own_ref, far_ref, tail_ref, ones_ref,
            points, fall, rise, spreads, own_points, own_fall, own_rise, ext, sums):
    segrows, share_rows, back, _, places = geo
    place = lax.axis_index("tm")
    diag = lax.axis_index("diag")

    odd = lax.rem(place, 2) == 1
    last = place == places - 1
    ext[segrows : 2 * segrows, :] = own_ref[...]

    @pl.when(odd)
    def _():
        ext[0:segrows, :] = near_ref[...]
        ext[2 * segrows : 3 * segrows, :] = far_ref[...]

    @pl.when(jnp.logical_not(odd))
    def _():
        ext[0:segrows, :] = far_ref[...]
        ext[2 * segrows : 3 * segrows, :] = near_ref[...]

    @pl.when(last)
    def _():
        tail_rows = M // LANES
        ext[2 * segrows : 2 * segrows + tail_rows, :] = tail_ref[...]
        ext[2 * segrows + tail_rows : 3 * segrows, :] = jnp.zeros(
            (segrows - tail_rows, LANES), jnp.float32
        )

    if ext.shape[0] > 3 * segrows:
        ext[3 * segrows :, :] = jnp.zeros((ext.shape[0] - 3 * segrows, LANES), jnp.float32)
    first_row = pl.multiple_of(segrows - back + share_rows * diag, SUB)
    points[...] = ext[pl.ds(first_row, 2 * LANES), :]

    ones = ones_ref[...]
    held = 2 * LANES - SUB

    def windows(values):
        sums[...] = window_pieces(values, ones)
        return (
            sums[0:held, 0:LANES]
            + (sums[1 : held + 1, 0:LANES] + sums[1 : held + 1, LANES:])
            + sums[2 : held + 2, LANES:]
        )

    x = points[...]
    mean = windows(x) * (1.0 / M)
    second = windows(x * x) * (1.0 / M)
    here = points[0:held, :]
    there = points[2 : held + 2, :]
    change = there - here
    pad = jnp.zeros((SUB, LANES), jnp.float32)
    spreads[0:held, :] = lax.rsqrt(second - mean * mean + 1e-05)
    fall[0:held, :] = 0.5 * change
    rise[0:held, :] = (there + here) - 2.0 * mean - change * (1.0 / M)
    for ref in (spreads, fall, rise):
        ref[held:, :] = pad

    chunks = share_rows // 2

    def own_rows(ref):
        halves = []
        for half in range(2):
            rows = ref[pl.ds(back + half, chunks, stride=2), :]
            halves.append(jnp.concatenate([rows] * (LANES // chunks), axis=0).T)
        return jnp.concatenate(halves, axis=0)

    turned = own_rows(points)
    own_points[...] = turned - jnp.sum(turned, axis=0, keepdims=True) * (1.0 / M)
    own_fall[...] = own_rows(fall)
    own_rise[...] = own_rows(rise)


def sweep(geo, offsets, excl, tables, scratch, before, best):
    points, fall, rise, spreads, own_points, own_fall, own_rise = tables
    moved, xband, fband, rband, sband, pband = scratch
    segrows, share_rows, back, _, places = geo
    place = lax.axis_index("tm")
    diag = lax.axis_index("diag")
    chunks = share_rows // 2

    lane = lax.broadcasted_iota(jnp.int32, (1, LANES), 1)
    sub = lax.broadcasted_iota(jnp.int32, (SUB, LANES), 0)
    lags = []
    for off in offsets:
        for lag in (off, -(off + (KB - 1))):
            lags += [lag, lag + HALF]
    first_lag = jnp.zeros((1, LANES), jnp.int32)
    for j, lag in enumerate(lags):
        first_lag = jnp.where(lane >= chunks * j, lag, first_lag)
    rows = moved.shape[2]

    def fill(n, ref, out):
        parts = [[] for _ in range(3)]
        for j, lag in enumerate(lags):
            base = back * LANES + lag
            row = lax.shift_right_logical(base, LANE_BITS)
            inner = base & (LANES - 1)
            turn = (LANES - inner) & (LANES - 1)
            moved[n, j] = pltpu.roll(ref[pl.ds(row, rows), :], turn, 1)
            near = lane < LANES - inner
            for q in range(3):
                parts[q].append(
                    jnp.where(
                        near,
                        moved[n, j, pl.ds(q, chunks, stride=2), :],
                        moved[n, j, pl.ds(q + 1, chunks, stride=2), :],
                    )
                )
        for q in range(3):
            held = min(LANES, BROWS - q * LANES)
            turned = jnp.concatenate(parts[q], axis=0).T
            out[q * LANES : q * LANES + held, :] = turned[0:held]

    def band(ref, start):
        return ref[pl.ds(start, SUB, stride=STEP), :]

    def row(ref, i):
        return ref[pl.ds(i, SUB, stride=0), :]

    fill(0, points, xband)
    totals = [None] * (TOTALS * STEP)
    for i in range(M):
        xi = row(own_points, i)
        for s in range(STEP):
            c = s + STEP * (i % TOTALS)
            term = xi * band(xband, i + s)
            totals[c] = term if totals[c] is None else totals[c] + term
    start = []
    for s in range(STEP):
        parts = list(totals[s::STEP])
        while len(parts) > 1:
            parts = [a + b for a, b in zip(parts[0::2], parts[1::2])]
        start.append(jnp.where(jnp.abs(first_lag + STEP * sub + s) < excl, -BIG, parts[0]))
    fill(1, spreads, sband)
    fill(2, fall, fband)
    fill(3, rise, rband)
    limit = places * segrows * LANES
    own_start = (place * segrows + share_rows * diag) * LANES
    position = own_start + (lane & (chunks - 1)) * M + first_lag
    position = position + lax.broadcasted_iota(jnp.int32, (BROWS, LANES), 0)
    pband[...] = jnp.where((position >= 0) & (position < limit), BIG, -BIG)

    def advance(step, covs):
        covs = list(covs)
        for u in range(UNROLL):
            i = step * UNROLL + u
            fi = row(own_fall, i)
            ri = row(own_rise, i)
            top = None if before is None else before[pl.ds(i, SUB, stride=SPAN), :]
            for s in range(STEP):
                value = jnp.minimum(covs[s] * band(sband, i + s), band(pband, i + s))
                top = value if top is None else jnp.maximum(top, value)
                covs[s] = covs[s] + (fi * band(rband, i + s) + ri * band(fband, i + s))
            best[pl.ds(i, SUB, stride=SPAN), :] = top
        return tuple(covs)

    lax.fori_loop(0, M // UNROLL, advance, tuple(start))


def picked(slots, groups):
    half = groups // 2
    return [slots[0, e] + slots[0, half + e] for e in range(half)]


def early(geo, mine_ref, *refs):
    tables, best, scratch = refs[:7], refs[7], refs[8:]
    slots = mine_ref[...]
    sweep(geo, picked(slots, geo[3]), slots[0, LANES - 1], tables, scratch, None, best)


def late(geo, mine_ref, other_ref, before, *refs):
    tables, out_ref, best, scratch = refs[:7], refs[7], refs[8], refs[9:]
    _, share_rows, back, groups, _ = geo
    chunks = share_rows // 2
    excl = mine_ref[0, LANES - 1]
    sweep(geo, picked(other_ref[...], groups), excl, tables, scratch, before, best)
    spreads = tables[3]

    for half in range(2):
        blocks = []
        for block in range(LANES // SUB):
            top = None
            for h in range(SUB):
                at = h * SPAN + half * LANES + block * SUB
                part = best[at : at + SUB, :]
                top = part if top is None else jnp.maximum(top, part)
            blocks.append(top)
        turned = jnp.concatenate(blocks, axis=0).T
        top = turned[0:chunks]
        for j in range(1, 2 * groups):
            top = jnp.maximum(top, turned[chunks * j : chunks * (j + 1)])
        spread = spreads[pl.ds(back + half, chunks, stride=2), :]
        distance = jnp.sqrt(jnp.maximum(1.0 - top * (spread * (1.0 / M)), 0.0))
        out_ref[pl.ds(half, chunks, stride=2), :] = jnp.where(top < -1e20, FILL, distance)


def on_device(series, tail, diag_offsets, exclusion):
    segment = series.shape[0]
    groups = lax.axis_size("diag")
    places = lax.axis_size("tm")
    reach = segment // 2 + segment // 4
    segrows = segment // LANES
    share_rows = segrows // groups
    back = reach // LANES
    deepest = segrows - back + share_rows * (groups - 1)
    geo = (segrows, share_rows, back, groups, places)
    f32 = jnp.float32
    rows = lambda a: a.reshape(-1, LANES)
    vmem = pl.BlockSpec(memory_space=pltpu.VMEM)
    mine, other = group_offsets(diag_offsets, exclusion)
    ones = pl.pallas_call(
        triangles,
        out_shape=jax.ShapeDtypeStruct((LANES, 2 * LANES), jnp.bfloat16),
        out_specs=vmem,
        compiler_params=pltpu.CompilerParams(vmem_limit_bytes=VMEM_LIMIT),
        cost_estimate=pl.CostEstimate(flops=COST_LOW, bytes_accessed=1 << 17, transcendentals=0),
        name="triangles",
    )()
    far = swapped(series, "tm", lambda i: i + 1 if i % 2 else i - 1)
    near = swapped(series, "tm", lambda i: i ^ 1)
    table = jax.ShapeDtypeStruct((2 * LANES, LANES), f32)
    tables = pl.pallas_call(
        functools.partial(prepare, geo),
        out_shape=[table] * 7,
        in_specs=[vmem] * 5,
        out_specs=[vmem] * 7,
        scratch_shapes=[
            pltpu.VMEM((max(3 * segrows, deepest + 2 * LANES), LANES), f32),
            pltpu.VMEM((2 * LANES, 2 * LANES), f32),
        ],
        compiler_params=pltpu.CompilerParams(vmem_limit_bytes=VMEM_LIMIT),
        cost_estimate=pl.CostEstimate(flops=COST_A, bytes_accessed=1 << 20, transcendentals=0),
        name="prepare",
    )(rows(near), rows(series), rows(far), rows(tail), ones)
    band = pltpu.VMEM((BROWS, LANES), f32)
    moved = pltpu.VMEM((4, 2 * groups, -(-(share_rows + 3) // SUB) * SUB, LANES), f32)
    scratch = [moved, band, band, band, band, band]
    params = pltpu.CompilerParams(vmem_limit_bytes=VMEM_LIMIT)
    maxima = pl.pallas_call(
        functools.partial(early, geo),
        out_shape=jax.ShapeDtypeStruct((SUB * SPAN, LANES), f32),
        in_specs=[vmem] * 8,
        out_specs=vmem,
        scratch_shapes=scratch,
        compiler_params=params,
        cost_estimate=pl.CostEstimate(flops=COST_A, bytes_accessed=1 << 20, transcendentals=0),
        name="early",
    )(rows(mine), *tables)
    out = pl.pallas_call(
        functools.partial(late, geo),
        out_shape=jax.ShapeDtypeStruct((share_rows, LANES), f32),
        in_specs=[vmem] * 10,
        out_specs=vmem,
        scratch_shapes=[pltpu.VMEM((SUB * SPAN, LANES), f32)] + scratch,
        compiler_params=params,
        cost_estimate=pl.CostEstimate(flops=1 << 24, bytes_accessed=1 << 20, transcendentals=0),
        name="late",
    )(rows(mine), rows(other), maxima, *tables)
    return out.reshape(-1)


def solution(mesh):
    in_specs = (P("tm"), P(), P("diag"), P())
    out_specs = P(("tm", "diag"))
    return jax.shard_map(
        on_device, mesh=mesh, in_specs=in_specs, out_specs=out_specs, check_vma=False
    )
```

```python
import functools

import jax
import jax.numpy as jnp
from jax import lax
from jax.experimental import pallas as pl
from jax.experimental.pallas import tpu as pltpu
from jax.sharding import PartitionSpec as P


M = 256
KB = 32
FILL = 1e30
LANES = 128
LANE_BITS = 7
SUB = 8
HALF = KB // 2
STEP = HALF // SUB
BROWS = M + HALF
SPAN = M + 4
BIG = 1e30
UNROLL = 64
TOTALS = 4
VMEM_LIMIT = 16 << 20
COST_A = 1 << 23
COST_LOW = 1 << 30


def swapped(shard, axis, partner):
    size = lax.axis_size(axis)
    return lax.ppermute(shard, axis, [(i, partner(i) % size) for i in range(size)])


def across(shard):
    places, groups = lax.axis_size("tm"), lax.axis_size("diag")

    def partner(i, d):
        other = i + 1 if i % 2 else i - 1
        return (other, d) if 0 <= other < places else (i, d ^ 1)

    pairs = []
    for i in range(places):
        for d in range(groups):
            other, group = partner(i, d)
            pairs.append((i * groups + d, other * groups + group))
    return lax.ppermute(shard, ("tm", "diag"), pairs)


def group_offsets(own, exclusion):
    size = lax.axis_size("diag")
    lanes = lax.iota(jnp.int32, LANES)
    slots = jnp.where(lanes == lax.axis_index("diag"), own[0], 0)
    other = jnp.zeros_like(slots)
    bit = 1
    while bit < size:
        slots = slots + other
        other = swapped(slots, "diag", lambda i: i ^ bit)
        bit *= 2
    return slots + jnp.where(lanes == LANES - 1, exclusion[0], 0), other


def split3(x):
    hi = x.astype(jnp.bfloat16)
    rest = x - hi.astype(jnp.float32)
    mid = rest.astype(jnp.bfloat16)
    low = (rest - mid.astype(jnp.float32)).astype(jnp.bfloat16)
    return hi, mid, low


def window_pieces(x, ones):
    out = None
    for piece in split3(x):
        part = jnp.dot(piece, ones, preferred_element_type=jnp.float32)
        out = part if out is None else out + part
    return out


def triangles(ones):
    rid = lax.broadcasted_iota(jnp.int32, (LANES, 2 * LANES), 0)
    cid = lax.broadcasted_iota(jnp.int32, (LANES, 2 * LANES), 1)
    ones[...] = jnp.where(
        cid < LANES, (rid >= cid).astype(jnp.float32), (rid < cid - LANES).astype(jnp.float32)
    ).astype(jnp.bfloat16)


def relay(back, source, own, near, far):
    rows = own.shape[0]
    own[...] = source[...]
    odd = lax.rem(lax.axis_index("tm"), 2) == 1

    @pl.when(odd)
    def _():
        near[...] = source[0:back, :]
        far[...] = source[rows - back : rows, :]

    @pl.when(jnp.logical_not(odd))
    def _():
        near[...] = source[rows - back : rows, :]
        far[...] = source[0:back, :]


def prepare(geo, near_ref, own_ref, far_ref, tail_ref, ones_ref,
            points, fall, rise, spreads, own_points, own_fall, own_rise, ext, sums):
    segrows, share_rows, back, _, places = geo
    place = lax.axis_index("tm")
    diag = lax.axis_index("diag")

    odd = lax.rem(place, 2) == 1
    last = place == places - 1
    ext[segrows : 2 * segrows, :] = own_ref[...]

    before, after = segrows - back, 2 * segrows + back

    @pl.when(odd)
    def _():
        ext[before:segrows, :] = near_ref[...]
        ext[2 * segrows : after, :] = far_ref[...]

    @pl.when(jnp.logical_not(odd))
    def _():
        ext[before:segrows, :] = far_ref[...]
        ext[2 * segrows : after, :] = near_ref[...]

    @pl.when(last)
    def _():
        tail_rows = M // LANES
        ext[2 * segrows : 2 * segrows + tail_rows, :] = tail_ref[...]
        ext[2 * segrows + tail_rows : after, :] = jnp.zeros((back - tail_rows, LANES), jnp.float32)

    ext[after:, :] = jnp.zeros((ext.shape[0] - after, LANES), jnp.float32)
    first_row = pl.multiple_of(segrows - back + share_rows * diag, SUB)
    points[...] = ext[pl.ds(first_row, 2 * LANES), :]

    ones = ones_ref[...]
    held = 2 * LANES - SUB

    def windows(values):
        sums[...] = window_pieces(values, ones)
        return (
            sums[0:held, 0:LANES]
            + (sums[1 : held + 1, 0:LANES] + sums[1 : held + 1, LANES:])
            + sums[2 : held + 2, LANES:]
        )

    x = points[...]
    mean = windows(x) * (1.0 / M)
    second = windows(x * x) * (1.0 / M)
    here = points[0:held, :]
    there = points[2 : held + 2, :]
    change = there - here
    pad = jnp.zeros((SUB, LANES), jnp.float32)
    spreads[0:held, :] = lax.rsqrt(second - mean * mean + 1e-05)
    fall[0:held, :] = 0.5 * change
    rise[0:held, :] = (there + here) - 2.0 * mean - change * (1.0 / M)
    for ref in (spreads, fall, rise):
        ref[held:, :] = pad

    chunks = share_rows // 2

    def own_rows(ref):
        halves = []
        for half in range(2):
            rows = ref[pl.ds(back + half, chunks, stride=2), :]
            halves.append(jnp.concatenate([rows] * (LANES // chunks), axis=0).T)
        return jnp.concatenate(halves, axis=0)

    turned = own_rows(points)
    own_points[...] = turned - jnp.sum(turned, axis=0, keepdims=True) * (1.0 / M)
    own_fall[...] = own_rows(fall)
    own_rise[...] = own_rows(rise)


def sweep(geo, offsets, excl, tables, scratch, before, best):
    points, fall, rise, spreads, own_points, own_fall, own_rise = tables
    moved, xband, fband, rband, sband, pband = scratch
    segrows, share_rows, back, _, places = geo
    place = lax.axis_index("tm")
    diag = lax.axis_index("diag")
    chunks = share_rows // 2

    lane = lax.broadcasted_iota(jnp.int32, (1, LANES), 1)
    sub = lax.broadcasted_iota(jnp.int32, (SUB, LANES), 0)
    lags = []
    for off in offsets:
        for lag in (off, -(off + (KB - 1))):
            lags += [lag, lag + HALF]
    first_lag = jnp.zeros((1, LANES), jnp.int32)
    for j, lag in enumerate(lags):
        first_lag = jnp.where(lane >= chunks * j, lag, first_lag)
    rows = moved.shape[2]

    def fill(n, ref, out):
        parts = [[] for _ in range(3)]
        for j, lag in enumerate(lags):
            base = back * LANES + lag
            row = lax.shift_right_logical(base, LANE_BITS)
            inner = base & (LANES - 1)
            turn = (LANES - inner) & (LANES - 1)
            moved[n, j] = pltpu.roll(ref[pl.ds(row, rows), :], turn, 1)
            near = lane < LANES - inner
            for q in range(3):
                parts[q].append(
                    jnp.where(
                        near,
                        moved[n, j, pl.ds(q, chunks, stride=2), :],
                        moved[n, j, pl.ds(q + 1, chunks, stride=2), :],
                    )
                )
        for q in range(3):
            held = min(LANES, BROWS - q * LANES)
            turned = jnp.concatenate(parts[q], axis=0).T
            out[q * LANES : q * LANES + held, :] = turned[0:held]

    def band(ref, start):
        return ref[pl.ds(start, SUB, stride=STEP), :]

    def row(ref, i):
        return ref[pl.ds(i, SUB, stride=0), :]

    fill(0, points, xband)
    totals = [None] * (TOTALS * STEP)
    for i in range(M):
        xi = row(own_points, i)
        for s in range(STEP):
            c = s + STEP * (i % TOTALS)
            term = xi * band(xband, i + s)
            totals[c] = term if totals[c] is None else totals[c] + term
    start = []
    for s in range(STEP):
        parts = list(totals[s::STEP])
        while len(parts) > 1:
            parts = [a + b for a, b in zip(parts[0::2], parts[1::2])]
        start.append(jnp.where(jnp.abs(first_lag + STEP * sub + s) < excl, -BIG, parts[0]))
    fill(1, spreads, sband)
    fill(2, fall, fband)
    fill(3, rise, rband)
    limit = places * segrows * LANES
    own_start = (place * segrows + share_rows * diag) * LANES
    position = own_start + (lane & (chunks - 1)) * M + first_lag
    position = position + lax.broadcasted_iota(jnp.int32, (BROWS, LANES), 0)
    pband[...] = jnp.where((position >= 0) & (position < limit), BIG, -BIG)

    def advance(step, covs):
        covs = list(covs)
        for u in range(UNROLL):
            i = step * UNROLL + u
            fi = row(own_fall, i)
            ri = row(own_rise, i)
            top = None if before is None else before[pl.ds(i, SUB, stride=SPAN), :]
            for s in range(STEP):
                value = jnp.minimum(covs[s] * band(sband, i + s), band(pband, i + s))
                top = value if top is None else jnp.maximum(top, value)
                covs[s] = covs[s] + (fi * band(rband, i + s) + ri * band(fband, i + s))
            best[pl.ds(i, SUB, stride=SPAN), :] = top
        return tuple(covs)

    lax.fori_loop(0, M // UNROLL, advance, tuple(start))


def picked(slots, groups):
    half = groups // 2
    return [slots[0, e] + slots[0, half + e] for e in range(half)]


def early(geo, mine_ref, *refs):
    tables, best, scratch = refs[:7], refs[7], refs[8:]
    slots = mine_ref[...]
    sweep(geo, picked(slots, geo[3]), slots[0, LANES - 1], tables, scratch, None, best)


def late(geo, mine_ref, other_ref, before, *refs):
    tables, out_ref, best, scratch = refs[:7], refs[7], refs[8], refs[9:]
    _, share_rows, back, groups, _ = geo
    chunks = share_rows // 2
    excl = mine_ref[0, LANES - 1]
    sweep(geo, picked(other_ref[...], groups), excl, tables, scratch, before, best)
    spreads = tables[3]

    for half in range(2):
        blocks = []
        for block in range(LANES // SUB):
            top = None
            for h in range(SUB):
                at = h * SPAN + half * LANES + block * SUB
                part = best[at : at + SUB, :]
                top = part if top is None else jnp.maximum(top, part)
            blocks.append(top)
        turned = jnp.concatenate(blocks, axis=0).T
        top = turned[0:chunks]
        for j in range(1, 2 * groups):
            top = jnp.maximum(top, turned[chunks * j : chunks * (j + 1)])
        spread = spreads[pl.ds(back + half, chunks, stride=2), :]
        distance = jnp.sqrt(jnp.maximum(1.0 - top * (spread * (1.0 / M)), 0.0))
        out_ref[pl.ds(half, chunks, stride=2), :] = jnp.where(top < -1e20, FILL, distance)


def on_device(series, tail, diag_offsets, exclusion):
    segment = series.shape[0]
    groups = lax.axis_size("diag")
    places = lax.axis_size("tm")
    reach = segment // 2 + segment // 4
    segrows = segment // LANES
    share_rows = segrows // groups
    back = reach // LANES
    deepest = segrows - back + share_rows * (groups - 1)
    geo = (segrows, share_rows, back, groups, places)
    f32 = jnp.float32
    rows = lambda a: a.reshape(-1, LANES)
    vmem = pl.BlockSpec(memory_space=pltpu.VMEM)
    mine, other = group_offsets(diag_offsets, exclusion)
    ones = pl.pallas_call(
        triangles,
        out_shape=jax.ShapeDtypeStruct((LANES, 2 * LANES), jnp.bfloat16),
        out_specs=vmem,
        compiler_params=pltpu.CompilerParams(vmem_limit_bytes=VMEM_LIMIT),
        cost_estimate=pl.CostEstimate(flops=COST_LOW, bytes_accessed=1 << 17, transcendentals=0),
        name="triangles",
    )()
    own, low, high = pl.pallas_call(
        functools.partial(relay, back),
        out_shape=[
            jax.ShapeDtypeStruct((segrows, LANES), f32),
            jax.ShapeDtypeStruct((back, LANES), f32),
            jax.ShapeDtypeStruct((back, LANES), f32),
        ],
        in_specs=[vmem],
        out_specs=[vmem] * 3,
        compiler_params=pltpu.CompilerParams(vmem_limit_bytes=VMEM_LIMIT),
        cost_estimate=pl.CostEstimate(flops=1 << 10, bytes_accessed=1 << 17, transcendentals=0),
        name="relay",
    )(rows(series))
    far = across(high)
    near = swapped(low, "tm", lambda i: i ^ 1)
    table = jax.ShapeDtypeStruct((2 * LANES, LANES), f32)
    tables = pl.pallas_call(
        functools.partial(prepare, geo),
        out_shape=[table] * 7,
        in_specs=[vmem] * 5,
        out_specs=[vmem] * 7,
        scratch_shapes=[
            pltpu.VMEM((max(3 * segrows, deepest + 2 * LANES), LANES), f32),
            pltpu.VMEM((2 * LANES, 2 * LANES), f32),
        ],
        compiler_params=pltpu.CompilerParams(vmem_limit_bytes=VMEM_LIMIT),
        cost_estimate=pl.CostEstimate(flops=COST_A, bytes_accessed=1 << 20, transcendentals=0),
        name="prepare",
    )(near, own, far, rows(tail), ones)
    band = pltpu.VMEM((BROWS, LANES), f32)
    moved = pltpu.VMEM((4, 2 * groups, -(-(share_rows + 3) // SUB) * SUB, LANES), f32)
    scratch = [moved, band, band, band, band, band]
    params = pltpu.CompilerParams(vmem_limit_bytes=VMEM_LIMIT)
    maxima = pl.pallas_call(
        functools.partial(early, geo),
        out_shape=jax.ShapeDtypeStruct((SUB * SPAN, LANES), f32),
        in_specs=[vmem] * 8,
        out_specs=vmem,
        scratch_shapes=scratch,
        compiler_params=params,
        cost_estimate=pl.CostEstimate(flops=COST_A, bytes_accessed=1 << 20, transcendentals=0),
        name="early",
    )(rows(mine), *tables)
    out = pl.pallas_call(
        functools.partial(late, geo),
        out_shape=jax.ShapeDtypeStruct((share_rows, LANES), f32),
        in_specs=[vmem] * 10,
        out_specs=vmem,
        scratch_shapes=[pltpu.VMEM((SUB * SPAN, LANES), f32)] + scratch,
        compiler_params=params,
        cost_estimate=pl.CostEstimate(flops=1 << 24, bytes_accessed=1 << 20, transcendentals=0),
        name="late",
    )(rows(mine), rows(other), maxima, *tables)
    return out.reshape(-1)


def solution(mesh):
    in_specs = (P("tm"), P(), P("diag"), P())
    out_specs = P(("tm", "diag"))
    return jax.shard_map(
        on_device, mesh=mesh, in_specs=in_specs, out_specs=out_specs, check_vma=False
    )
```

```python
import functools

import jax
import jax.numpy as jnp
from jax import lax
from jax.experimental import pallas as pl
from jax.experimental.pallas import tpu as pltpu
from jax.sharding import PartitionSpec as P


M = 256
KB = 32
FILL = 1e30
LANES = 128
LANE_BITS = 7
SUB = 8
HALF = KB // 2
STEP = HALF // SUB
BROWS = M + HALF
SPAN = M + 4
BIG = 1e30
UNROLL = 64
TOTALS = 4
VMEM_LIMIT = 16 << 20
COST_A = 1 << 23
COST_LOW = 1 << 30


def swapped(shard, axis, partner):
    size = lax.axis_size(axis)
    return lax.ppermute(shard, axis, [(i, partner(i) % size) for i in range(size)])


def across(shard):
    places, groups = lax.axis_size("tm"), lax.axis_size("diag")

    def partner(i, d):
        other = i + 1 if i % 2 else i - 1
        return (other, d) if 0 <= other < places else (i, d ^ 1)

    pairs = []
    for i in range(places):
        for d in range(groups):
            other, group = partner(i, d)
            pairs.append((i * groups + d, other * groups + group))
    return lax.ppermute(shard, ("tm", "diag"), pairs)


def group_offsets(own, exclusion):
    size = lax.axis_size("diag")
    lanes = lax.iota(jnp.int32, LANES)
    slots = jnp.where(lanes == lax.axis_index("diag"), own[0], 0)
    other = jnp.zeros_like(slots)
    bit = 1
    while bit < size:
        slots = slots + other
        other = swapped(slots, "diag", lambda i: i ^ bit)
        bit *= 2
    return slots + jnp.where(lanes == LANES - 1, exclusion[0], 0), other


def split3(x):
    hi = x.astype(jnp.bfloat16)
    rest = x - hi.astype(jnp.float32)
    mid = rest.astype(jnp.bfloat16)
    low = (rest - mid.astype(jnp.float32)).astype(jnp.bfloat16)
    return hi, mid, low


def window_pieces(x, ones):
    out = None
    for piece in split3(x):
        part = jnp.dot(piece, ones, preferred_element_type=jnp.float32)
        out = part if out is None else out + part
    return out


def triangles(ones):
    rid = lax.broadcasted_iota(jnp.int32, (LANES, 2 * LANES), 0)
    cid = lax.broadcasted_iota(jnp.int32, (LANES, 2 * LANES), 1)
    ones[...] = jnp.where(
        cid < LANES, (rid >= cid).astype(jnp.float32), (rid < cid - LANES).astype(jnp.float32)
    ).astype(jnp.bfloat16)


def relay(back, source, own, near, far):
    rows = own.shape[0]
    own[...] = source[...]
    odd = lax.rem(lax.axis_index("tm"), 2) == 1

    @pl.when(odd)
    def _():
        near[...] = source[0:back, :]
        far[...] = source[rows - back : rows, :]

    @pl.when(jnp.logical_not(odd))
    def _():
        near[...] = source[rows - back : rows, :]
        far[...] = source[0:back, :]


def prepare(geo, near_ref, own_ref, far_ref, tail_ref, ones_ref,
            points, fall, rise, spreads, own_points, own_fall, own_rise, ext, sums):
    segrows, share_rows, back, _, places = geo
    place = lax.axis_index("tm")
    diag = lax.axis_index("diag")

    odd = lax.rem(place, 2) == 1
    last = place == places - 1
    ext[segrows : 2 * segrows, :] = own_ref[...]

    before, after = segrows - back, 2 * segrows + back

    @pl.when(odd)
    def _():
        ext[before:segrows, :] = near_ref[...]
        ext[2 * segrows : after, :] = far_ref[...]

    @pl.when(jnp.logical_not(odd))
    def _():
        ext[before:segrows, :] = far_ref[...]
        ext[2 * segrows : after, :] = near_ref[...]

    @pl.when(last)
    def _():
        tail_rows = M // LANES
        ext[2 * segrows : 2 * segrows + tail_rows, :] = tail_ref[...]
        ext[2 * segrows + tail_rows : after, :] = jnp.zeros((back - tail_rows, LANES), jnp.float32)

    ext[after:, :] = jnp.zeros((ext.shape[0] - after, LANES), jnp.float32)
    first_row = pl.multiple_of(segrows - back + share_rows * diag, SUB)
    points[...] = ext[pl.ds(first_row, 2 * LANES), :]

    ones = ones_ref[...]
    held = 2 * LANES - SUB

    def windows(values):
        sums[...] = window_pieces(values, ones)
        return (
            sums[0:held, 0:LANES]
            + (sums[1 : held + 1, 0:LANES] + sums[1 : held + 1, LANES:])
            + sums[2 : held + 2, LANES:]
        )

    x = points[...]
    mean = windows(x) * (1.0 / M)
    second = windows(x * x) * (1.0 / M)
    here = points[0:held, :]
    there = points[2 : held + 2, :]
    change = there - here
    pad = jnp.zeros((SUB, LANES), jnp.float32)
    spreads[0:held, :] = lax.rsqrt(second - mean * mean + 1e-05)
    fall[0:held, :] = 0.5 * change
    rise[0:held, :] = (there + here) - 2.0 * mean - change * (1.0 / M)
    for ref in (spreads, fall, rise):
        ref[held:, :] = pad

    chunks = share_rows // 2

    def own_rows(ref):
        halves = []
        for half in range(2):
            rows = ref[pl.ds(back + half, chunks, stride=2), :]
            halves.append(jnp.concatenate([rows] * (LANES // chunks), axis=0).T)
        return jnp.concatenate(halves, axis=0)

    turned = own_rows(points)
    own_points[...] = turned - jnp.sum(turned, axis=0, keepdims=True) * (1.0 / M)
    own_fall[...] = own_rows(fall)
    own_rise[...] = own_rows(rise)


def sweep(geo, offsets, excl, tables, scratch, before, best):
    points, fall, rise, spreads, own_points, own_fall, own_rise = tables
    moved, xband, fband, rband, sband, pband = scratch
    segrows, share_rows, back, _, places = geo
    place = lax.axis_index("tm")
    diag = lax.axis_index("diag")
    chunks = share_rows // 2

    lane = lax.broadcasted_iota(jnp.int32, (1, LANES), 1)
    sub = lax.broadcasted_iota(jnp.int32, (SUB, LANES), 0)
    firsts = []
    for off in offsets:
        firsts += [off, -(off + (KB - 1))]
    lags = firsts + [lag + HALF for lag in firsts]
    first_lag = jnp.zeros((1, LANES), jnp.int32)
    for j, lag in enumerate(lags):
        first_lag = jnp.where(lane >= chunks * j, lag, first_lag)
    rows = moved.shape[2]

    def fill(n, ref, out):
        parts = [[] for _ in range(3)]
        for j, lag in enumerate(firsts):
            base = back * LANES + lag
            row = lax.shift_right_logical(base, LANE_BITS)
            inner = base & (LANES - 1)
            turn = (LANES - inner) & (LANES - 1)
            moved[n, j] = pltpu.roll(ref[pl.ds(row, rows), :], turn, 1)
            near = lane < LANES - inner
            for q in range(3):
                parts[q].append(
                    jnp.where(
                        near,
                        moved[n, j, pl.ds(q, chunks, stride=2), :],
                        moved[n, j, pl.ds(q + 1, chunks, stride=2), :],
                    )
                )
        turned = [jnp.concatenate(parts[q] * 2, axis=0).T for q in range(3)]
        whole = jnp.concatenate([turned[0], turned[1], turned[2][0 : 2 * HALF]], axis=0)
        out[...] = jnp.where(lane < LANES // 2, whole[0:BROWS], whole[HALF : BROWS + HALF])

    def band(ref, start):
        return ref[pl.ds(start, SUB, stride=STEP), :]

    def row(ref, i):
        return ref[pl.ds(i, SUB, stride=0), :]

    fill(0, points, xband)
    totals = [None] * (TOTALS * STEP)
    for i in range(M):
        xi = row(own_points, i)
        for s in range(STEP):
            c = s + STEP * (i % TOTALS)
            term = xi * band(xband, i + s)
            totals[c] = term if totals[c] is None else totals[c] + term
    start = []
    for s in range(STEP):
        parts = list(totals[s::STEP])
        while len(parts) > 1:
            parts = [a + b for a, b in zip(parts[0::2], parts[1::2])]
        start.append(jnp.where(jnp.abs(first_lag + STEP * sub + s) < excl, -BIG, parts[0]))
    fill(1, spreads, sband)
    fill(2, fall, fband)
    fill(3, rise, rband)
    limit = places * segrows * LANES
    own_start = (place * segrows + share_rows * diag) * LANES
    position = own_start + (lane & (chunks - 1)) * M + first_lag
    position = position + lax.broadcasted_iota(jnp.int32, (BROWS, LANES), 0)
    pband[...] = jnp.where((position >= 0) & (position < limit), BIG, -BIG)

    def advance(step, covs):
        covs = list(covs)
        for u in range(UNROLL):
            i = step * UNROLL + u
            fi = row(own_fall, i)
            ri = row(own_rise, i)
            top = None if before is None else before[pl.ds(i, SUB, stride=SPAN), :]
            for s in range(STEP):
                value = jnp.minimum(covs[s] * band(sband, i + s), band(pband, i + s))
                top = value if top is None else jnp.maximum(top, value)
                covs[s] = covs[s] + (fi * band(rband, i + s) + ri * band(fband, i + s))
            best[pl.ds(i, SUB, stride=SPAN), :] = top
        return tuple(covs)

    lax.fori_loop(0, M // UNROLL, advance, tuple(start))


def picked(slots, groups):
    half = groups // 2
    return [slots[0, e] + slots[0, half + e] for e in range(half)]


def early(geo, mine_ref, *refs):
    tables, best, scratch = refs[:7], refs[7], refs[8:]
    slots = mine_ref[...]
    sweep(geo, picked(slots, geo[3]), slots[0, LANES - 1], tables, scratch, None, best)


def late(geo, mine_ref, other_ref, before, *refs):
    tables, out_ref, best, scratch = refs[:7], refs[7], refs[8], refs[9:]
    _, share_rows, back, groups, _ = geo
    chunks = share_rows // 2
    excl = mine_ref[0, LANES - 1]
    sweep(geo, picked(other_ref[...], groups), excl, tables, scratch, before, best)
    spreads = tables[3]

    for half in range(2):
        blocks = []
        for block in range(LANES // SUB):
            top = None
            for h in range(SUB):
                at = h * SPAN + half * LANES + block * SUB
                part = best[at : at + SUB, :]
                top = part if top is None else jnp.maximum(top, part)
            blocks.append(top)
        turned = jnp.concatenate(blocks, axis=0).T
        top = turned[0:chunks]
        for j in range(1, 2 * groups):
            top = jnp.maximum(top, turned[chunks * j : chunks * (j + 1)])
        spread = spreads[pl.ds(back + half, chunks, stride=2), :]
        distance = jnp.sqrt(jnp.maximum(1.0 - top * (spread * (1.0 / M)), 0.0))
        out_ref[pl.ds(half, chunks, stride=2), :] = jnp.where(top < -1e20, FILL, distance)


def on_device(series, tail, diag_offsets, exclusion):
    segment = series.shape[0]
    groups = lax.axis_size("diag")
    places = lax.axis_size("tm")
    reach = segment // 2 + segment // 4
    segrows = segment // LANES
    share_rows = segrows // groups
    back = reach // LANES
    deepest = segrows - back + share_rows * (groups - 1)
    geo = (segrows, share_rows, back, groups, places)
    f32 = jnp.float32
    rows = lambda a: a.reshape(-1, LANES)
    vmem = pl.BlockSpec(memory_space=pltpu.VMEM)
    mine, other = group_offsets(diag_offsets, exclusion)
    ones = pl.pallas_call(
        triangles,
        out_shape=jax.ShapeDtypeStruct((LANES, 2 * LANES), jnp.bfloat16),
        out_specs=vmem,
        compiler_params=pltpu.CompilerParams(vmem_limit_bytes=VMEM_LIMIT),
        cost_estimate=pl.CostEstimate(flops=COST_LOW, bytes_accessed=1 << 17, transcendentals=0),
        name="triangles",
    )()
    own, low, high = pl.pallas_call(
        functools.partial(relay, back),
        out_shape=[
            jax.ShapeDtypeStruct((segrows, LANES), f32),
            jax.ShapeDtypeStruct((back, LANES), f32),
            jax.ShapeDtypeStruct((back, LANES), f32),
        ],
        in_specs=[vmem],
        out_specs=[vmem] * 3,
        compiler_params=pltpu.CompilerParams(vmem_limit_bytes=VMEM_LIMIT),
        cost_estimate=pl.CostEstimate(flops=1 << 10, bytes_accessed=1 << 17, transcendentals=0),
        name="relay",
    )(rows(series))
    far = across(high)
    near = swapped(low, "tm", lambda i: i ^ 1)
    table = jax.ShapeDtypeStruct((2 * LANES, LANES), f32)
    tables = pl.pallas_call(
        functools.partial(prepare, geo),
        out_shape=[table] * 7,
        in_specs=[vmem] * 5,
        out_specs=[vmem] * 7,
        scratch_shapes=[
            pltpu.VMEM((max(3 * segrows, deepest + 2 * LANES), LANES), f32),
            pltpu.VMEM((2 * LANES, 2 * LANES), f32),
        ],
        compiler_params=pltpu.CompilerParams(vmem_limit_bytes=VMEM_LIMIT),
        cost_estimate=pl.CostEstimate(flops=COST_A, bytes_accessed=1 << 20, transcendentals=0),
        name="prepare",
    )(near, own, far, rows(tail), ones)
    band = pltpu.VMEM((BROWS, LANES), f32)
    moved = pltpu.VMEM((4, groups, -(-(share_rows + 3) // SUB) * SUB, LANES), f32)
    scratch = [moved, band, band, band, band, band]
    params = pltpu.CompilerParams(vmem_limit_bytes=VMEM_LIMIT)
    maxima = pl.pallas_call(
        functools.partial(early, geo),
        out_shape=jax.ShapeDtypeStruct((SUB * SPAN, LANES), f32),
        in_specs=[vmem] * 8,
        out_specs=vmem,
        scratch_shapes=scratch,
        compiler_params=params,
        cost_estimate=pl.CostEstimate(flops=COST_A, bytes_accessed=1 << 20, transcendentals=0),
        name="early",
    )(rows(mine), *tables)
    out = pl.pallas_call(
        functools.partial(late, geo),
        out_shape=jax.ShapeDtypeStruct((share_rows, LANES), f32),
        in_specs=[vmem] * 10,
        out_specs=vmem,
        scratch_shapes=[pltpu.VMEM((SUB * SPAN, LANES), f32)] + scratch,
        compiler_params=params,
        cost_estimate=pl.CostEstimate(flops=1 << 24, bytes_accessed=1 << 20, transcendentals=0),
        name="late",
    )(rows(mine), rows(other), maxima, *tables)
    return out.reshape(-1)


def solution(mesh):
    in_specs = (P("tm"), P(), P("diag"), P())
    out_specs = P(("tm", "diag"))
    return jax.shard_map(
        on_device, mesh=mesh, in_specs=in_specs, out_specs=out_specs, check_vma=False
    )
```
